32 devices in a mesh: dp: 2 (over x), fsdp: 16 (over z, y, core).
Axes of the slice: x: 2, y: 2, z: 4, core: 2. Of those that a mesh axis runs over, the one named last changes fastest.
Arguments:
- group_grads: bfloat16 [2, 46, 512, 512], P('dp', None, 'fsdp')
- owners: int32 [46, 1], replicated, may hold values from 0 to 15; in each aligned block of 46 rows (0 to 45, 46 to 91, ...) at most 8 rows name the same one
- stats_left: float32 [16, 8, 512, 512], P('fsdp', 'dp'), as said below
- stats_right: float32 [16, 8, 512, 512], P('fsdp', 'dp'), as said below
Outputs:
- preconditioned: bfloat16 [46, 512, 512], P(None, 'fsdp')
The draws below stay inside these ranges and needn't reach their ends.
Inputs may be any that keep to these rules, and one draw needn't show every extreme that they name: `owners`: no owner names more than 8 blocks, some owner names exactly 8, and every owner 0 to 15 names at least one block. `stats_left`: each [512, 512] matrix is symmetric positive definite. `stats_right`: each [512, 512] matrix is symmetric positive definite.
All inputs are finite; a program needn't handle non-finite values.
Results may differ from the reference program's by a relative error of at most 0.017.
Values may be sent and summed in bfloat16 or wider, within the bound.
A program may use at most 64 MiB of HBM per device.

```python
import math
import jax
import jax.numpy as jnp
import numpy as np
from jax import lax

B = 512
MOST = 8
ITERS = 2
NBLK = 46
N_DP = 2
N_FSDP = 16


def entries_of(key, shape):
    return jax.random.normal(key, shape, jnp.float32)


def decaying_product(key, falloff_width, scale):
    former_key, latter_key = jax.random.split(key)
    former = entries_of(former_key, (B, B))
    latter = entries_of(latter_key, (B, B))
    falloff = 1.0 / (1.0 + jnp.arange(B, dtype=jnp.float32) / falloff_width)
    joined = jnp.dot(former * falloff[None, :], latter, precision=lax.Precision.HIGHEST, preferred_element_type=jnp.float32)
    return joined * (scale / jnp.sqrt(jnp.sum(falloff * falloff)))


def stat_law(key):
    weight = 12.0
    ridge_eye = 0.01 * B * jnp.eye(B, dtype=jnp.float32)

    def one_matrix(matrix_index):
        past_grads = decaying_product(jax.random.fold_in(key, matrix_index), 16.0, 1.0)
        gram_matrix = jnp.dot(past_grads, past_grads.T, precision=lax.Precision.HIGHEST, preferred_element_type=jnp.float32)
        return weight * 0.5 * (gram_matrix + gram_matrix.T) + ridge_eye
    stacked_stats = lax.map(one_matrix, jnp.arange(N_FSDP * MOST, dtype=jnp.int32))
    return stacked_stats.reshape(N_FSDP, MOST, B, B)


def draw_stats_left(key, part):
    return stat_law(jax.random.fold_in(key, 11))


def draw_stats_right(key, part):
    return stat_law(jax.random.fold_in(key, 23))


def draw_group_grads(key, part):
    mixing_key = jax.random.fold_in(key, 37)
    noise_key = jax.random.fold_in(key, 41)

    def one_block(block_index):
        mixing = decaying_product(jax.random.fold_in(mixing_key, block_index), 2.0, B ** (-0.5))
        fresh_terms = entries_of(jax.random.fold_in(noise_key, block_index), (N_DP, B, B))
        mixed_terms = jnp.einsum('gij,jk->gik', fresh_terms, mixing, precision=lax.Precision.HIGHEST, preferred_element_type=jnp.float32)
        return (mixed_terms * N_DP ** (-0.5)).astype(jnp.bfloat16)
    blocks = lax.map(one_block, jnp.arange(NBLK, dtype=jnp.int32))
    return jnp.swapaxes(blocks, 0, 1)


def shared_out(own_key, own, number, rows, amount, top, limit, slope):
    sequence = jax.random.permutation(own_key, amount)
    packed, ordinary = portions_of(amount, rows * top, limit, slope, True), portions_of(amount, rows * top, limit, slope, False)
    places = jnp.arange(amount)

    def named(sizes, turn):
        used = int((sizes > 0).sum())
        fixed = max(1, used // 4)
        moved = fixed + (places - fixed + turn * (used - fixed)) % max(1, amount - fixed)
        return jnp.zeros((amount,), jnp.int32).at[sequence[jnp.where(places < fixed, places, moved)]].set(jnp.asarray(sizes, jnp.int32))

    sizes = jnp.where(number % 4 == 0, named(packed, number // 4), named(ordinary, number - number // 4 - 1))
    mixed = jax.random.permutation(jax.random.fold_in(own, 3), amount)
    source_of, receiver = mixed[0:amount // 2 * 2:2], mixed[1:amount // 2 * 2:2]
    margin = jnp.minimum(sizes[source_of] - 1, limit - sizes[receiver]) // 2
    margin = jnp.where((source_of == sequence[0]) | (receiver == sequence[0]) | (sizes[receiver] == 0), 0, jnp.maximum(margin, 0))
    moved = jax.random.randint(jax.random.fold_in(own, 4), (amount // 2,), 0, 1 << 20) % (margin + 1)
    sizes = sizes.at[source_of].add(-moved).at[receiver].add(moved)
    members = jnp.searchsorted(jnp.cumsum(sizes), jnp.arange(rows * top), side="right").astype(jnp.int32)
    table = members.reshape(top, rows).T
    table = table[jax.random.permutation(jax.random.fold_in(own, 1), rows)]
    turn = jax.random.randint(jax.random.fold_in(own, 2), (rows, 1), 0, top)
    return jnp.take_along_axis(table, (jnp.arange(top)[None, :] + turn) % top, axis=1)


def portions_of(count, total, reach, skew, full):
    loads = [(1 << 20) // math.isqrt(grade ** skew) + 1 for grade in range(1, count + 1)]
    largest = reach if full else min(reach, max(-(-total // count), total * loads[0] // sum(loads)))
    least = 1 if total - largest >= count - 1 else 0
    given, surplus = [largest] + [least] * (count - 1), total - largest - least * (count - 1)
    while surplus > 0:
        free = [i for i in range(1, count) if given[i] < largest] or [i for i in range(1, count) if given[i] < reach]
        mass, remaining = sum([loads[i] for i in free]), surplus
        for i in free:
            more = min(reach - given[i], max(1, remaining * loads[i] // mass), surplus)
            given[i] = given[i] + more
            surplus = surplus - more
    return np.array(given)


def setup_inputs(seed: int = 0) -> dict:
    key_list = jax.random.split(jax.random.key(seed), 5)
    group_grads = draw_group_grads(jax.random.fold_in(key_list[4], 71), 0)
    owners_keys = jax.random.split(jax.random.fold_in(key_list[1], 1), NBLK // NBLK)
    owners_turns = jax.random.permutation(jax.random.fold_in(key_list[1], 3), NBLK // NBLK)
    owners = jax.vmap(lambda own, number: shared_out(jax.random.fold_in(key_list[1], 2), own, number, NBLK, N_FSDP, 1, MOST, 2))(owners_keys, owners_turns).reshape((NBLK, 1))
    stats_left = draw_stats_left(jax.random.fold_in(key_list[4], 71), 0)
    stats_right = draw_stats_right(jax.random.fold_in(key_list[4], 71), 0)
    return dict(group_grads=group_grads, owners=owners, stats_left=stats_left, stats_right=stats_right)


BETA = 0.95

def product(former, latter):
    return jnp.dot(former, latter, precision=lax.Precision.HIGHEST, preferred_element_type=jnp.float32)

def newton_root(statistic):
    identity = jnp.eye(statistic.shape[0], dtype=statistic.dtype)
    magnitude = jnp.sqrt(jnp.sum(statistic * statistic) + 1e-06)
    moment = statistic / magnitude
    factor = identity
    for iteration in range(ITERS):
        correction = (5.0 * identity - moment) * 0.25
        if iteration == 0:
            factor = correction
        else:
            factor = product(factor, correction)
        if iteration + 1 < ITERS:
            square = product(correction, correction)
            fourth = product(square, square)
            moment = product(fourth, moment)
    return factor

def reference(group_grads, owners, stats_left, stats_right):
    owner_of = owners[:, 0]
    positions = jnp.arange(owner_of.shape[0], dtype=jnp.int32)
    earlier = (owner_of[None, :] == owner_of[:, None]) & (positions[None, :] < positions[:, None])
    slot_of = lax.optimization_barrier(jnp.sum(earlier.astype(jnp.int32), axis=1)).astype(jnp.int32)

    def process_block(block_id):
        pieces = lax.dynamic_index_in_dim(group_grads, block_id, axis=1, keepdims=False)
        gradient = lax.optimization_barrier(jnp.sum(pieces.astype(jnp.float32), axis=0)).astype(jnp.bfloat16)
        left_old = stats_left[owner_of[block_id], slot_of[block_id]]
        right_old = stats_right[owner_of[block_id], slot_of[block_id]]
        left_stat = BETA * left_old + jnp.dot(gradient, gradient.T, preferred_element_type=jnp.float32)
        right_stat = BETA * right_old + jnp.dot(gradient.T, gradient, preferred_element_type=jnp.float32)
        left_root = newton_root(left_stat).astype(jnp.bfloat16)
        right_root = newton_root(right_stat).astype(jnp.bfloat16)
        halfway = jnp.dot(left_root, gradient, preferred_element_type=jnp.float32).astype(jnp.bfloat16)
        shaped = jnp.dot(halfway, right_root, preferred_element_type=jnp.float32)
        graft_ratio = jnp.sqrt(jnp.sum(jnp.square(gradient.astype(jnp.float32)))) / jnp.sqrt(jnp.sum(shaped * shaped) + 1e-06)
        return (shaped * graft_ratio).astype(jnp.bfloat16)
    return lax.map(process_block, positions)
```

```python
import functools
import math
import jax
import jax.numpy as jnp
from jax import lax
from jax.experimental import pallas as pl
from jax.experimental.pallas import tpu as pltpu
from jax.sharding import PartitionSpec as P

ITERS = 2


BETA = 0.95

POWER = [math.comb(5, j) * 5.0 ** (5 - j) * (-1.0) ** j / 4.0**6 for j in range(6)]
COEF = [25.0 / 16.0, -5.0 / 16.0 - POWER[0]] + [-POWER[j] for j in range(1, 6)]


def mm(former, latter, dims=((1,), (0,))):
    return lax.dot_general(former, latter, (dims, ((), ())), preferred_element_type=jnp.float32)


def total_of(value):
    return jnp.sum(jnp.sum(value, axis=0, keepdims=True), axis=1, keepdims=True)


def newton_root(statistic):
    magnitude = jnp.sqrt(total_of(statistic * statistic) + 1e-06)
    first = statistic * (1.0 / magnitude)
    low_first = first.astype(jnp.bfloat16)
    second = mm(low_first, low_first)
    third = mm(second.astype(jnp.bfloat16), low_first)
    upper = COEF[4] * first + COEF[5] * second + COEF[6] * third
    lower = COEF[1] * first + COEF[2] * second + COEF[3] * third
    factor = lower + mm(third.astype(jnp.bfloat16), upper.astype(jnp.bfloat16))
    row = lax.broadcasted_iota(jnp.int32, factor.shape, 0)
    column = lax.broadcasted_iota(jnp.int32, factor.shape, 1)
    return (factor + jnp.where(row == column, COEF[0], 0.0)).astype(jnp.bfloat16)


def shape_kernel(gradient_ref, left_ref, right_ref, update_ref):
    gradient = gradient_ref[0]
    left_root = newton_root(BETA * left_ref[0] + mm(gradient, gradient, ((1,), (1,))))
    halfway = mm(left_root, gradient).astype(jnp.bfloat16)
    right_root = newton_root(BETA * right_ref[0] + mm(gradient, gradient, ((0,), (0,))))
    shaped = mm(halfway, right_root)
    wide = gradient.astype(jnp.float32)
    ratio = jnp.sqrt(total_of(wide * wide)) / jnp.sqrt(total_of(shaped * shaped) + 1e-06)
    update_ref[0] = (shaped * ratio).astype(jnp.bfloat16)


def shape_blocks(gradient, left, right, interpret=False):
    count, width, _ = gradient.shape
    spec = pl.BlockSpec((1, width, width), lambda k: (k, 0, 0))
    return pl.pallas_call(
        shape_kernel,
        grid=(count,),
        out_shape=jax.ShapeDtypeStruct(gradient.shape, jnp.bfloat16),
        in_specs=[spec] * 3,
        out_specs=spec,
        compiler_params=pltpu.CompilerParams(vmem_limit_bytes=48 * 1024 * 1024),
        cost_estimate=pl.CostEstimate(
            flops=20 * count * width**3, bytes_accessed=12 * count * width**2, transcendentals=0
        ),
        interpret=interpret,
    )(gradient, left, right)


def shifted(value, groups, step):
    return lax.ppermute(value, "dp", [(g, (g + step) % groups) for g in range(groups)])


def slot_table(owners):
    owner_of = owners[:, 0]
    positions = jnp.arange(owner_of.shape[0], dtype=jnp.int32)
    earlier = (owner_of[None, :] == owner_of[:, None]) & (positions[None, :] < positions[:, None])
    slot_of = jnp.sum(earlier.astype(jnp.int32), axis=1)
    return (owner_of, slot_of, positions)

MESH = pl.DeviceIdType.MESH


def shape_block(gradient, left, right):
    left_root = newton_root(BETA * left + mm(gradient, gradient, ((1,), (1,))))
    halfway = mm(left_root, gradient).astype(jnp.bfloat16)
    right_root = newton_root(BETA * right + mm(gradient, gradient, ((0,), (0,))))
    shaped = mm(halfway, right_root)
    wide = gradient.astype(jnp.float32)
    ratio = jnp.sqrt(total_of(wide * wide)) / jnp.sqrt(total_of(shaped * shaped) + 1e-06)
    return (shaped * ratio).astype(jnp.bfloat16)


def level_caps(blocks, shards, capacity, levels):
    caps = [shards]
    for slot in range(1, levels):
        caps.append(min(shards, (blocks - capacity + slot + 1 - shards) // slot))
    return caps


def fused_kernel(
    caps,
    send_block,
    own_block,
    own_rank,
    pack_owner,
    pick,
    grads,
    left_hbm,
    right_hbm,
    out,
    left,
    right,
    x_out,
    summed,
    gradient,
    update,
    settled,
    back_out,
    stat_sem,
    x_send,
    x_recv,
    in_send,
    in_recv,
    out_send,
    out_recv,
    back_send,
    back_recv,
    *landing,
):
    levels = len(caps)
    x_in, result = landing[:levels], landing[levels:]
    starts = [sum(caps[:s]) for s in range(levels)]
    shards, rows, width = gradient.shape[1:]
    group, me = lax.axis_index("dp"), lax.axis_index("fsdp")
    partner = (1 - group, me)

    def stat_copies(s):
        return [
            pltpu.make_async_copy(left_hbm.at[s], left.at[s], stat_sem.at[0, s]),
            pltpu.make_async_copy(right_hbm.at[s], right.at[s], stat_sem.at[1, s]),
        ]

    for s in range(levels):
        for copy in stat_copies(s):
            copy.start()

    barrier = pltpu.get_barrier_semaphore()
    pl.semaphore_signal(barrier, inc=1, device_id=partner, device_id_type=MESH)

    @pl.loop(1, shards)
    def _(k):
        pl.semaphore_signal(
            barrier, inc=1, device_id=(group, lax.rem(me + k, shards)), device_id_type=MESH
        )

    def x_copy(s):
        part = pl.ds(starts[s], caps[s])
        return pltpu.make_async_remote_copy(
            src_ref=x_out.at[part],
            dst_ref=x_in[s],
            send_sem=x_send.at[s],
            recv_sem=x_recv.at[s],
            device_id=partner,
            device_id_type=MESH,
        )

    def fill(s):
        for i in range(caps[s]):
            x_out[starts[s] + i] = grads[send_block[s, i]]

    fill(0)
    pl.semaphore_wait(barrier, shards)
    x_copy(0).start()
    for s in range(1, levels):
        fill(s)
        x_copy(s).start()

    def in_copy(s, k):
        owner = lax.rem(me + k, shards)
        return pltpu.make_async_remote_copy(
            src_ref=summed.at[s, owner],
            dst_ref=gradient.at[s, me],
            send_sem=in_send.at[s, k],
            recv_sem=in_recv.at[s, k],
            device_id=(group, owner),
            device_id_type=MESH,
        )

    def out_copy(s, k):
        shard = lax.rem(me + k, shards)
        return pltpu.make_async_remote_copy(
            src_ref=update.at[s, shard],
            dst_ref=result[s].at[me],
            send_sem=out_send.at[s, k],
            recv_sem=out_recv.at[s, k],
            device_id=(group, shard),
            device_id_type=MESH,
        )

    def back_copy(s):
        part = pl.ds(starts[s], caps[s])
        return pltpu.make_async_remote_copy(
            src_ref=back_out.at[part],
            dst_ref=settled.at[pl.ds(levels * shards + starts[s], caps[s])],
            send_sem=back_send.at[s],
            recv_sem=back_recv.at[s],
            device_id=partner,
            device_id_type=MESH,
        )

    def scatter(s):
        x_copy(s).wait_recv()

        @pl.loop(0, shards)
        def _(o):
            mine = grads[own_block[s, o]].astype(jnp.float32)
            theirs = x_in[s][own_rank[s, o]].astype(jnp.float32)
            summed[s, o] = (mine + theirs).astype(jnp.bfloat16)

        gradient[s, me] = summed[s, me]

        @pl.loop(1, shards)
        def _(k):
            in_copy(s, k).start()

    def compute(s):
        @pl.loop(1, shards)
        def _(k):
            in_copy(s, k).wait_recv()

        for copy in stat_copies(s):
            copy.wait()
        block = gradient[s].reshape(shards * rows, width)
        update[s] = shape_block(block, left[s], right[s]).reshape(shards, rows, width)

    def spread(s):
        result[s][me] = update[s, me]

        @pl.loop(1, shards)
        def _(k):
            out_copy(s, k).start()

    def give_back(s):
        @pl.loop(1, shards)
        def _(k):
            out_copy(s, k).wait_recv()

        for i in range(caps[s]):
            back_out[starts[s] + i] = result[s][pack_owner[s, i]]
        back_copy(s).start()
        for o in range(shards):
            settled[s * shards + o] = result[s][o]

    ahead = min(2, levels)
    for s in range(ahead):
        scatter(s)

    @pl.loop(0, levels)
    def _(step):
        compute(step)
        for s in range(levels):

            @pl.when(step == s)
            def _():
                spread(s)

        for s in range(ahead, levels):

            @pl.when(step == s - ahead)
            def _():
                scatter(s)

        for s in range(levels - 1):

            @pl.when(step == s + 1)
            def _():
                give_back(s)

    give_back(levels - 1)
    for s in range(levels):
        back_copy(s).wait_recv()
    for b in range(out.shape[0]):
        out[b] = settled[pick[b]]
    for s in range(levels):

        @pl.loop(1, shards)
        def _(k):
            in_copy(s, k).wait_send()
            out_copy(s, k).wait_send()

        x_copy(s).wait_send()
        back_copy(s).wait_send()


def pair_tables(owners, member, shards, levels, caps):
    owner_of, slot_of, positions = slot_table(owners)
    slots = jnp.arange(2 * levels, dtype=jnp.int32)
    names = jnp.arange(shards, dtype=jnp.int32)
    matches = (slot_of[None, None, :] == slots[:, None, None]) & (
        owner_of[None, None, :] == names[None, :, None]
    )
    block = jnp.sum(jnp.where(matches, positions, 0), axis=2)
    count = jnp.sum((owner_of[None, :] == names[:, None]).astype(jnp.int32), axis=1)
    present = count[None, :] > slots[:, None]
    before = names[None, :] < names[:, None]
    rank = jnp.sum((present[:, None, :] & before[None]).astype(jnp.int32), axis=2)
    rank = jnp.where(present, rank, 0)
    places = jnp.arange(max(caps), dtype=jnp.int32)
    at_place = present[:, None, :] & (rank[:, None, :] == places[None, :, None])
    place_block = jnp.sum(jnp.where(at_place, block[:, None, :], 0), axis=2)
    place_owner = jnp.sum(jnp.where(at_place, names, 0), axis=2)

    def side(table, which):
        return lax.dynamic_slice_in_dim(table, which * levels, levels, 0)

    level = slot_of % levels
    start = sum(jnp.where(level > s, caps[s], 0) for s in range(levels))
    ahead_of = (count[None, :] > slot_of[:, None]) & (names[None, :] < owner_of[:, None])
    block_rank = jnp.sum(ahead_of.astype(jnp.int32), axis=1)
    pick = jnp.where(
        slot_of // levels == member,
        level * shards + owner_of,
        levels * shards + start + block_rank,
    )
    return (
        side(place_block, 1 - member),
        side(block, member),
        side(rank, member),
        side(place_owner, member),
        pick,
    )


def pair_body(group_grads, owners, stats_left, stats_right):
    shards = lax.axis_size("fsdp")
    member = lax.axis_index("dp")
    _, blocks, rows, width = group_grads.shape
    levels = stats_left.shape[1]
    caps = level_caps(blocks, shards, 2 * levels, levels)
    tables = pair_tables(owners, member, shards, levels, caps)
    piece = (rows, width)
    dma = pltpu.SemaphoreType.DMA
    bf16 = jnp.bfloat16
    vmem = pl.BlockSpec(memory_space=pltpu.VMEM)
    smem = pl.BlockSpec(memory_space=pltpu.SMEM)
    anywhere = pl.BlockSpec(memory_space=pl.ANY)
    return pl.pallas_call(
        functools.partial(fused_kernel, caps),
        out_shape=jax.ShapeDtypeStruct((blocks, *piece), bf16),
        in_specs=[smem] * 5 + [vmem, anywhere, anywhere],
        out_specs=vmem,
        scratch_shapes=[
            pltpu.VMEM((levels, width, width), jnp.float32),
            pltpu.VMEM((levels, width, width), jnp.float32),
            pltpu.VMEM((sum(caps), *piece), bf16),
            pltpu.VMEM((levels, shards, *piece), bf16),
            pltpu.VMEM((levels, shards, *piece), bf16),
            pltpu.VMEM((levels, shards, *piece), bf16),
            pltpu.VMEM((levels * shards + sum(caps), *piece), bf16),
            pltpu.VMEM((sum(caps), *piece), bf16),
            dma((2, levels)),
            dma((levels,)),
            dma((levels,)),
            dma((levels, shards)),
            dma((levels, shards)),
            dma((levels, shards)),
            dma((levels, shards)),
            dma((levels,)),
            dma((levels,)),
        ]
        + [pltpu.VMEM((cap, *piece), bf16) for cap in caps]
        + [pltpu.VMEM((shards, *piece), bf16)] * levels,
        compiler_params=pltpu.CompilerParams(
            collective_id=0, has_side_effects=True, vmem_limit_bytes=56 * 1024 * 1024
        ),
    )(*tables, group_grads[0], stats_left[0], stats_right[0])


def body(group_grads, owners, stats_left, stats_right):
    groups = lax.axis_size("dp")
    member = lax.axis_index("dp")
    shards = lax.axis_size("fsdp")
    per_member = stats_left.shape[1]
    capacity = per_member * groups
    owner_of, slot_of, positions = slot_table(owners)
    local = group_grads[0]
    total = local.astype(jnp.float32)
    for step in range(1, groups):
        total = total + shifted(local, groups, step).astype(jnp.float32)
    summed = total.astype(jnp.bfloat16)
    rows_here = summed.shape[1]
    block_width = summed.shape[2]
    wanted = member * per_member + jnp.arange(per_member, dtype=jnp.int32)
    targets = (jnp.arange(shards, dtype=jnp.int32)[:, None] * capacity + wanted[None, :]).reshape(
        -1
    )
    block_key = owner_of * capacity + slot_of
    matches = targets[:, None] == block_key[None, :]
    present = jnp.any(matches, axis=1)
    chosen = jnp.sum(jnp.where(matches, positions[None, :], 0), axis=1)
    outgoing = jnp.where(
        present[:, None, None], jnp.take(summed, chosen, axis=0), jnp.zeros((), jnp.bfloat16)
    )
    outgoing = outgoing.reshape(shards, per_member, rows_here, block_width)
    arrived = lax.all_to_all(outgoing, "fsdp", split_axis=0, concat_axis=2, tiled=True)
    gradient = arrived.reshape(per_member, block_width, block_width)
    update = shape_blocks(gradient, stats_left[0], stats_right[0])
    pieces = update.reshape(per_member, shards, rows_here, block_width)
    returned = lax.all_to_all(pieces, "fsdp", split_axis=1, concat_axis=0, tiled=True)
    returned = returned.reshape(shards * per_member, rows_here, block_width)
    mine = jnp.take(returned, owner_of * per_member + slot_of % per_member, axis=0)
    holder = slot_of // per_member
    result = mine
    for step in range(1, groups):
        theirs = (holder == (member - step) % groups)[:, None, None]
        result = jnp.where(theirs, shifted(mine, groups, step), result)
    return result


def solution(mesh):
    placed = (
        P("dp", None, "fsdp", None),
        P(),
        P("fsdp", "dp", None, None),
        P("fsdp", "dp", None, None),
    )
    return jax.shard_map(
        pair_body if mesh.shape["dp"] == 2 else body, mesh=mesh, in_specs=placed, out_specs=P(None, "fsdp", None), check_vma=False
    )
```

```python
import functools
import math
import jax
import jax.numpy as jnp
from jax import lax
from jax.experimental import pallas as pl
from jax.experimental.pallas import tpu as pltpu
from jax.sharding import PartitionSpec as P

ITERS = 2


BETA = 0.95
AHEAD = 3

POWER = [math.comb(5, j) * 5.0 ** (5 - j) * (-1.0) ** j / 4.0**6 for j in range(6)]
COEF = [25.0 / 16.0, -5.0 / 16.0 - POWER[0]] + [-POWER[j] for j in range(1, 6)]


def mm(former, latter, dims=((1,), (0,))):
    return lax.dot_general(former, latter, (dims, ((), ())), preferred_element_type=jnp.float32)


def total_of(value):
    return jnp.sum(jnp.sum(value, axis=0, keepdims=True), axis=1, keepdims=True)


def newton_root(statistic):
    magnitude = jnp.sqrt(total_of(statistic * statistic) + 1e-06)
    first = statistic * (1.0 / magnitude)
    low_first = first.astype(jnp.bfloat16)
    second = mm(low_first, low_first)
    third = mm(second.astype(jnp.bfloat16), low_first)
    upper = COEF[4] * first + COEF[5] * second + COEF[6] * third
    lower = COEF[1] * first + COEF[2] * second + COEF[3] * third
    factor = lower + mm(third.astype(jnp.bfloat16), upper.astype(jnp.bfloat16))
    row = lax.broadcasted_iota(jnp.int32, factor.shape, 0)
    column = lax.broadcasted_iota(jnp.int32, factor.shape, 1)
    return (factor + jnp.where(row == column, COEF[0], 0.0)).astype(jnp.bfloat16)


def shape_kernel(gradient_ref, left_ref, right_ref, update_ref):
    gradient = gradient_ref[0]
    left_root = newton_root(BETA * left_ref[0] + mm(gradient, gradient, ((1,), (1,))))
    halfway = mm(left_root, gradient).astype(jnp.bfloat16)
    right_root = newton_root(BETA * right_ref[0] + mm(gradient, gradient, ((0,), (0,))))
    shaped = mm(halfway, right_root)
    wide = gradient.astype(jnp.float32)
    ratio = jnp.sqrt(total_of(wide * wide)) / jnp.sqrt(total_of(shaped * shaped) + 1e-06)
    update_ref[0] = (shaped * ratio).astype(jnp.bfloat16)


def shape_blocks(gradient, left, right, interpret=False):
    count, width, _ = gradient.shape
    spec = pl.BlockSpec((1, width, width), lambda k: (k, 0, 0))
    return pl.pallas_call(
        shape_kernel,
        grid=(count,),
        out_shape=jax.ShapeDtypeStruct(gradient.shape, jnp.bfloat16),
        in_specs=[spec] * 3,
        out_specs=spec,
        compiler_params=pltpu.CompilerParams(vmem_limit_bytes=48 * 1024 * 1024),
        cost_estimate=pl.CostEstimate(
            flops=20 * count * width**3, bytes_accessed=12 * count * width**2, transcendentals=0
        ),
        interpret=interpret,
    )(gradient, left, right)


def shifted(value, groups, step):
    return lax.ppermute(value, "dp", [(g, (g + step) % groups) for g in range(groups)])


def slot_table(owners):
    owner_of = owners[:, 0]
    positions = jnp.arange(owner_of.shape[0], dtype=jnp.int32)
    earlier = (owner_of[None, :] == owner_of[:, None]) & (positions[None, :] < positions[:, None])
    slot_of = jnp.sum(earlier.astype(jnp.int32), axis=1)
    return (owner_of, slot_of, positions)

MESH = pl.DeviceIdType.MESH


def shape_block(gradient, left, right):
    left_root = newton_root(BETA * left + mm(gradient, gradient, ((1,), (1,))))
    halfway = mm(left_root, gradient).astype(jnp.bfloat16)
    right_root = newton_root(BETA * right + mm(gradient, gradient, ((0,), (0,))))
    shaped = mm(halfway, right_root)
    wide = gradient.astype(jnp.float32)
    ratio = jnp.sqrt(total_of(wide * wide)) / jnp.sqrt(total_of(shaped * shaped) + 1e-06)
    return (shaped * ratio).astype(jnp.bfloat16)


def level_caps(blocks, shards, capacity, levels):
    caps = [shards]
    for slot in range(1, levels):
        caps.append(min(shards, (blocks - capacity + slot + 1 - shards) // slot))
    return caps


def visit_order(shards):
    stride = next(s for s in range(math.isqrt(shards), 0, -1) if shards % s == 0)
    return stride, [o for r in range(stride) for o in range(r, shards, stride)]


def table_kernel(levels, shards, caps, owners_ref, table_ref):
    blocks = owners_ref.shape[1]
    stride, _ = visit_order(shards)

    def numbers(shape, axis):
        return lax.broadcasted_iota(jnp.int32, shape, axis).astype(jnp.float32)

    def split(value, size):
        quotient = jnp.floor((value + 0.5) * (1.0 / size))
        return quotient, value - size * quotient

    def visit(owner):
        quotient, rest = split(owner, stride)
        return rest * (shards // stride) + quotient

    def down(mask, value=1.0):
        return jnp.sum(jnp.where(mask, value, 0.0), axis=0, keepdims=True)

    def across(mask, value=1.0):
        return jnp.sum(jnp.where(mask, value, 0.0), axis=1, keepdims=True)

    square = (blocks, blocks)
    first, second = numbers(square, 0), numbers(square, 1)
    owner_row = owners_ref[...].astype(jnp.float32)
    owner_col = across(first == second, owner_row)
    same = owner_col == owner_row
    slot_row = down(same & (first < second))
    slot_col = across(same & (second < first))
    visit_row, visit_col = visit(owner_row), visit(owner_col)
    level = slot_col == slot_row
    rank_row = down(level & (visit_col < visit_row))
    rank_col = across(level & (visit_row < visit_col))
    wide = (blocks, 2 * levels * shards)
    slot, place = split(numbers(wide, 1), shards)
    at_owner = (slot_col == slot) & (owner_col == place)
    at_place = (slot_col == slot) & (rank_col == place)
    block_col = numbers(wide, 0)
    rows = [
        down(at_owner, block_col),
        down(at_owner, rank_col),
        down(at_place, block_col),
        down(at_place, owner_col),
    ]
    for r, row in enumerate(rows):
        table_ref[r : r + 1, 0 : wide[1]] = row.astype(jnp.int32)
    holder, depth = split(slot_row, levels)
    start = sum(jnp.where(depth > s, float(caps[s]), 0.0) for s in range(levels))
    place_row = rank_row
    for s in range(levels):
        if caps[s] == shards:
            place_row = jnp.where(depth == s, owner_row, place_row)
    for member in range(2):
        pick = jnp.where(
            holder == member, depth * shards + owner_row, levels * shards + start + place_row
        )
        table_ref[4 + member : 5 + member, 0:blocks] = pick.astype(jnp.int32)


def fused_kernel(
    caps,
    table,
    grads,
    left_hbm,
    right_hbm,
    settled,
    left,
    right,
    x_out,
    summed,
    gradient,
    update,
    back_out,
    stat_sem,
    x_send,
    x_recv,
    in_send,
    in_recv,
    out_send,
    out_recv,
    back_send,
    back_recv,
    *landing,
):
    levels = len(caps)
    x_in, result, back_in = landing[:levels], landing[levels : 2 * levels], landing[2 * levels]
    starts = [sum(caps[:s]) for s in range(levels)]
    shards, rows, width = gradient.shape[1:]
    full = [cap == shards for cap in caps]
    stride, order = visit_order(shards)
    part = shards // stride
    parts = [(0, i, part) for i in range(0, shards, part)]
    parts += [(s, 0, caps[s]) for s in range(1, levels)]
    group, me = lax.axis_index("dp"), lax.axis_index("fsdp")
    partner = (1 - group, me)

    def lookup(row, side, s, i):
        return table[row, (side * levels + s) * shards + i]

    def stat_copies(s):
        return [
            pltpu.make_async_copy(left_hbm.at[s], left.at[s], stat_sem.at[0, s]),
            pltpu.make_async_copy(right_hbm.at[s], right.at[s], stat_sem.at[1, s]),
        ]

    barrier = pltpu.get_barrier_semaphore()
    pl.semaphore_signal(barrier, inc=1, device_id=partner, device_id_type=MESH)

    @pl.loop(1, shards)
    def _(k):
        pl.semaphore_signal(
            barrier, inc=1, device_id=(group, lax.rem(me + k, shards)), device_id_type=MESH
        )

    for s in range(levels):
        for copy in stat_copies(s):
            copy.start()

    def x_copy(n):
        s, i, size = parts[n]
        return pltpu.make_async_remote_copy(
            src_ref=x_out.at[pl.ds(starts[s] + i, size)],
            dst_ref=x_in[s].at[pl.ds(i, size)],
            send_sem=x_send.at[n],
            recv_sem=x_recv.at[n],
            device_id=partner,
            device_id_type=MESH,
        )

    def fill(n):
        s, first, size = parts[n]
        for i in range(first, first + size):
            block = lookup(0, 1 - group, s, order[i]) if full[s] else lookup(2, 1 - group, s, i)
            x_out[starts[s] + i] = grads[block]

    fill(0)
    pl.semaphore_wait(barrier, shards)
    for n in range(len(parts)):
        x_copy(n).start()
        if n + 1 < len(parts):
            fill(n + 1)

    def in_copy(s, owner, source):
        return pltpu.make_async_remote_copy(
            src_ref=summed.at[s, owner],
            dst_ref=gradient.at[s, source],
            send_sem=in_send.at[s, owner],
            recv_sem=in_recv.at[s, source],
            device_id=(group, owner),
            device_id_type=MESH,
        )

    def out_copy(s, shard, source):
        return pltpu.make_async_remote_copy(
            src_ref=update.at[s, shard],
            dst_ref=result[s].at[source],
            send_sem=out_send.at[s, shard],
            recv_sem=out_recv.at[s, source],
            device_id=(group, shard),
            device_id_type=MESH,
        )

    def back_copy(s):
        part = pl.ds(starts[s], caps[s])
        return pltpu.make_async_remote_copy(
            src_ref=result[s] if full[s] else back_out.at[part],
            dst_ref=back_in.at[part],
            send_sem=back_send.at[s],
            recv_sem=back_recv.at[s],
            device_id=partner,
            device_id_type=MESH,
        )

    def other(k):
        return lax.rem(me + k, shards)

    def added(s, owner, theirs):
        mine = grads[lookup(0, group, s, owner)].astype(jnp.float32)
        summed[s, owner] = (mine + theirs.astype(jnp.float32)).astype(jnp.bfloat16)

    def scatter_first():
        for n in range(stride):
            x_copy(n).wait_recv()
            here = range(n * part, (n + 1) * part)
            for i in here:
                added(0, order[i], x_in[0][i])
            for i in here:
                owner = order[i]

                @pl.when(owner != me)
                def _():
                    in_copy(0, owner, me).start()

        gradient[0, me] = summed[0, me]

    def scatter(s):
        x_copy(stride + s - 1).wait_recv()

        if full[s]:
            for i in range(shards):
                added(s, order[i], x_in[s][i])
        else:

            @pl.loop(0, shards)
            def _(o):
                added(s, o, x_in[s][lookup(1, group, s, o)])

        gradient[s, me] = summed[s, me]

        @pl.loop(1, shards)
        def _(k):
            in_copy(s, other(k), me).start()

    def compute(s):
        @pl.loop(1, shards)
        def _(k):
            in_copy(s, me, other(k)).wait_recv()

        for copy in stat_copies(s):
            copy.wait()
        block = gradient[s].reshape(shards * rows, width)
        update[s] = shape_block(block, left[s], right[s]).reshape(shards, rows, width)

    def spread(s):
        result[s][me] = update[s, me]

        @pl.loop(1, shards)
        def _(k):
            out_copy(s, other(k), me).start()

    def give_back(s):
        @pl.loop(1, shards)
        def _(k):
            out_copy(s, me, other(k)).wait_recv()

        if not full[s]:
            for i in range(caps[s]):
                back_out[starts[s] + i] = result[s][lookup(3, group, s, i)]
        back_copy(s).start()
        for o in range(shards):
            settled[s * shards + o] = result[s][o]

    ahead = min(AHEAD, levels)
    scatter_first()
    for s in range(1, ahead):
        scatter(s)

    @pl.loop(0, levels)
    def _(step):
        compute(step)
        for s in range(levels):

            @pl.when(step == s)
            def _():
                spread(s)

        for s in range(ahead, levels):

            @pl.when(step == s - ahead)
            def _():
                scatter(s)

        for s in range(levels - 1):

            @pl.when(step == s + 1)
            def _():
                give_back(s)

    give_back(levels - 1)
    for s in range(levels):
        back_copy(s).wait_recv()
        for i in range(caps[s]):
            settled[levels * shards + starts[s] + i] = back_in[starts[s] + i]
    for s in range(levels):

        @pl.loop(1, shards)
        def _(k):
            in_copy(s, other(k), me).wait_send()
            out_copy(s, other(k), me).wait_send()

        back_copy(s).wait_send()
    for n in range(len(parts)):
        x_copy(n).wait_send()


def settle_kernel(table, settled, out):
    member = lax.axis_index("dp")
    for b in range(out.shape[0]):
        out[b] = settled[table[4 + member, b]]


def pair_body(group_grads, owners, stats_left, stats_right):
    shards = lax.axis_size("fsdp")
    _, blocks, rows, width = group_grads.shape
    levels = stats_left.shape[1]
    caps = level_caps(blocks, shards, 2 * levels, levels)
    piece = (rows, width)
    dma = pltpu.SemaphoreType.DMA
    bf16 = jnp.bfloat16
    vmem = pl.BlockSpec(memory_space=pltpu.VMEM)
    smem = pl.BlockSpec(memory_space=pltpu.SMEM)
    anywhere = pl.BlockSpec(memory_space=pl.ANY)
    table = pl.pallas_call(
        functools.partial(table_kernel, levels, shards, caps),
        out_shape=jax.ShapeDtypeStruct((8, max(2 * levels * shards, blocks)), jnp.int32),
        in_specs=[vmem],
        out_specs=vmem,
    )(owners.reshape(1, blocks))
    messages = visit_order(shards)[0] + levels - 1
    settled = pl.pallas_call(
        functools.partial(fused_kernel, caps),
        out_shape=jax.ShapeDtypeStruct((levels * shards + sum(caps), *piece), bf16),
        in_specs=[smem, vmem, anywhere, anywhere],
        out_specs=vmem,
        scratch_shapes=[
            pltpu.VMEM((levels, width, width), jnp.float32),
            pltpu.VMEM((levels, width, width), jnp.float32),
            pltpu.VMEM((sum(caps), *piece), bf16),
            pltpu.VMEM((levels, shards, *piece), bf16),
            pltpu.VMEM((levels, shards, *piece), bf16),
            pltpu.VMEM((levels, shards, *piece), bf16),
            pltpu.VMEM((sum(caps), *piece), bf16),
            dma((2, levels)),
            dma((messages,)),
            dma((messages,)),
            dma((levels, shards)),
            dma((levels, shards)),
            dma((levels, shards)),
            dma((levels, shards)),
            dma((levels,)),
            dma((levels,)),
        ]
        + [pltpu.VMEM((cap, *piece), bf16) for cap in caps]
        + [pltpu.VMEM((shards, *piece), bf16)] * levels
        + [pltpu.VMEM((sum(caps), *piece), bf16)],
        compiler_params=pltpu.CompilerParams(
            collective_id=0, has_side_effects=True, vmem_limit_bytes=48 * 1024 * 1024
        ),
    )(table, group_grads[0], stats_left[0], stats_right[0])
    return pl.pallas_call(
        settle_kernel,
        out_shape=jax.ShapeDtypeStruct((blocks, *piece), bf16),
        in_specs=[smem, vmem],
        out_specs=vmem,
        compiler_params=pltpu.CompilerParams(vmem_limit_bytes=16 * 1024 * 1024),
    )(table, settled)


def body(group_grads, owners, stats_left, stats_right):
    groups = lax.axis_size("dp")
    member = lax.axis_index("dp")
    shards = lax.axis_size("fsdp")
    per_member = stats_left.shape[1]
    capacity = per_member * groups
    owner_of, slot_of, positions = slot_table(owners)
    local = group_grads[0]
    total = local.astype(jnp.float32)
    for step in range(1, groups):
        total = total + shifted(local, groups, step).astype(jnp.float32)
    summed = total.astype(jnp.bfloat16)
    rows_here = summed.shape[1]
    block_width = summed.shape[2]
    wanted = member * per_member + jnp.arange(per_member, dtype=jnp.int32)
    targets = (jnp.arange(shards, dtype=jnp.int32)[:, None] * capacity + wanted[None, :]).reshape(
        -1
    )
    block_key = owner_of * capacity + slot_of
    matches = targets[:, None] == block_key[None, :]
    present = jnp.any(matches, axis=1)
    chosen = jnp.sum(jnp.where(matches, positions[None, :], 0), axis=1)
    outgoing = jnp.where(
        present[:, None, None], jnp.take(summed, chosen, axis=0), jnp.zeros((), jnp.bfloat16)
    )
    outgoing = outgoing.reshape(shards, per_member, rows_here, block_width)
    arrived = lax.all_to_all(outgoing, "fsdp", split_axis=0, concat_axis=2, tiled=True)
    gradient = arrived.reshape(per_member, block_width, block_width)
    update = shape_blocks(gradient, stats_left[0], stats_right[0])
    pieces = update.reshape(per_member, shards, rows_here, block_width)
    returned = lax.all_to_all(pieces, "fsdp", split_axis=1, concat_axis=0, tiled=True)
    returned = returned.reshape(shards * per_member, rows_here, block_width)
    mine = jnp.take(returned, owner_of * per_member + slot_of % per_member, axis=0)
    holder = slot_of // per_member
    result = mine
    for step in range(1, groups):
        theirs = (holder == (member - step) % groups)[:, None, None]
        result = jnp.where(theirs, shifted(mine, groups, step), result)
    return result


def solution(mesh):
    placed = (
        P("dp", None, "fsdp", None),
        P(),
        P("fsdp", "dp", None, None),
        P("fsdp", "dp", None, None),
    )
    return jax.shard_map(
        pair_body if mesh.shape["dp"] == 2 else body, mesh=mesh, in_specs=placed, out_specs=P(None, "fsdp", None), check_vma=False
    )
```

```python
import functools
import math
import jax
import jax.numpy as jnp
from jax import lax
from jax.experimental import pallas as pl
from jax.experimental.pallas import tpu as pltpu
from jax.sharding import PartitionSpec as P

ITERS = 2


BETA = 0.95

POWER = [math.comb(5, j) * 5.0 ** (5 - j) * (-1.0) ** j / 4.0**6 for j in range(6)]
COEF = [25.0 / 16.0, -5.0 / 16.0 - POWER[0]] + [-POWER[j] for j in range(1, 6)]


def mm(former, latter, dims=((1,), (0,))):
    return lax.dot_general(former, latter, (dims, ((), ())), preferred_element_type=jnp.float32)


def total_of(value):
    return jnp.sum(jnp.sum(value, axis=0, keepdims=True), axis=1, keepdims=True)


def newton_root(statistic):
    magnitude = jnp.sqrt(total_of(statistic * statistic) + 1e-06)
    first = statistic * (1.0 / magnitude)
    low_first = first.astype(jnp.bfloat16)
    second = mm(low_first, low_first)
    third = mm(second.astype(jnp.bfloat16), low_first)
    upper = COEF[4] * first + COEF[5] * second + COEF[6] * third
    lower = COEF[1] * first + COEF[2] * second + COEF[3] * third
    factor = lower + mm(third.astype(jnp.bfloat16), upper.astype(jnp.bfloat16))
    row = lax.broadcasted_iota(jnp.int32, factor.shape, 0)
    column = lax.broadcasted_iota(jnp.int32, factor.shape, 1)
    return (factor + jnp.where(row == column, COEF[0], 0.0)).astype(jnp.bfloat16)


def shape_kernel(gradient_ref, left_ref, right_ref, update_ref):
    gradient = gradient_ref[0]
    left_root = newton_root(BETA * left_ref[0] + mm(gradient, gradient, ((1,), (1,))))
    halfway = mm(left_root, gradient).astype(jnp.bfloat16)
    right_root = newton_root(BETA * right_ref[0] + mm(gradient, gradient, ((0,), (0,))))
    shaped = mm(halfway, right_root)
    wide = gradient.astype(jnp.float32)
    ratio = jnp.sqrt(total_of(wide * wide)) / jnp.sqrt(total_of(shaped * shaped) + 1e-06)
    update_ref[0] = (shaped * ratio).astype(jnp.bfloat16)


def shape_blocks(gradient, left, right, interpret=False):
    count, width, _ = gradient.shape
    spec = pl.BlockSpec((1, width, width), lambda k: (k, 0, 0))
    return pl.pallas_call(
        shape_kernel,
        grid=(count,),
        out_shape=jax.ShapeDtypeStruct(gradient.shape, jnp.bfloat16),
        in_specs=[spec] * 3,
        out_specs=spec,
        compiler_params=pltpu.CompilerParams(vmem_limit_bytes=48 * 1024 * 1024),
        cost_estimate=pl.CostEstimate(
            flops=20 * count * width**3, bytes_accessed=12 * count * width**2, transcendentals=0
        ),
        interpret=interpret,
    )(gradient, left, right)


def shifted(value, groups, step):
    return lax.ppermute(value, "dp", [(g, (g + step) % groups) for g in range(groups)])


def slot_table(owners):
    owner_of = owners[:, 0]
    positions = jnp.arange(owner_of.shape[0], dtype=jnp.int32)
    earlier = (owner_of[None, :] == owner_of[:, None]) & (positions[None, :] < positions[:, None])
    slot_of = jnp.sum(earlier.astype(jnp.int32), axis=1)
    return (owner_of, slot_of, positions)

MESH = pl.DeviceIdType.MESH


def shape_block(gradient, left, right):
    left_root = newton_root(BETA * left + mm(gradient, gradient, ((1,), (1,))))
    halfway = mm(left_root, gradient).astype(jnp.bfloat16)
    right_root = newton_root(BETA * right + mm(gradient, gradient, ((0,), (0,))))
    shaped = mm(halfway, right_root)
    wide = gradient.astype(jnp.float32)
    ratio = jnp.sqrt(total_of(wide * wide)) / jnp.sqrt(total_of(shaped * shaped) + 1e-06)
    return (shaped * ratio).astype(jnp.bfloat16)


def level_caps(blocks, shards, capacity, levels):
    caps = [shards]
    for slot in range(1, levels):
        caps.append(min(shards, (blocks - capacity + slot + 1 - shards) // slot))
    return caps


def stride_of(shards):
    return next(s for s in range(math.isqrt(shards), 0, -1) if shards % s == 0)


def table_kernel(light, heavy, shards, owners_ref, table_ref):
    blocks = owners_ref.shape[1]
    levels = light + heavy
    stride = stride_of(shards)
    part = shards // stride
    longest = stride * heavy

    def numbers(shape, axis):
        return lax.broadcasted_iota(jnp.int32, shape, axis).astype(jnp.float32)

    def split(value, size):
        quotient = jnp.floor((value + 0.5) * (1.0 / size))
        return quotient, value - size * quotient

    def down(mask, value=1.0):
        return jnp.sum(jnp.where(mask, value, 0.0), axis=0, keepdims=True)

    def across(mask, value=1.0):
        return jnp.sum(jnp.where(mask, value, 0.0), axis=1, keepdims=True)

    def listed(owner, slot):
        holder, depth = split(slot, levels)
        ring, rest = split(owner, stride)
        name = jnp.where(depth >= light, holder * part + ring, -1.0)
        return name, depth * stride + rest

    square = (blocks, blocks)
    first, second = numbers(square, 0), numbers(square, 1)
    owner_row = owners_ref[...].astype(jnp.float32)
    owner_col = across(first == second, owner_row)
    same = owner_col == owner_row
    slot_row = down(same & (first < second))
    slot_col = across(same & (second < first))
    list_row, key_row = listed(owner_row, slot_row)
    list_col, key_col = listed(owner_col, slot_col)
    together = list_col == list_row
    rank_row = down(together & (key_col < key_row))
    rank_col = across(together & (key_row < key_col))
    wide = (blocks, 2 * levels * shards)
    slot, owner = split(numbers(wide, 1), shards)
    at_owner = (slot_col == slot) & (owner_col == owner)
    block_col = numbers(wide, 0)
    lists = (blocks, 2 * part * longest)
    name, place = split(numbers(lists, 1), longest)
    at_place = (list_col == name) & (rank_col == place)
    rows = [
        down(at_owner, block_col),
        down(at_owner & (list_col >= 0.0), rank_col),
        down(at_place, numbers(lists, 0)),
        down(at_place, key_col - light * stride),
    ]
    for r, row in enumerate(rows):
        table_ref[r : r + 1, 0 : row.shape[1]] = row.astype(jnp.int32)
    holder, depth = split(slot_row, levels)
    ring, rest = split(owner_row, stride)
    near = jnp.where(
        list_row < 0.0,
        depth * shards + rest * part + ring,
        light * shards + ring * longest + rank_row,
    )
    side = light * shards + part * longest
    for member in range(2):
        pick = near + jnp.where(holder == member, 0.0, float(side))
        table_ref[4 + member : 5 + member, 0:blocks] = pick.astype(jnp.int32)
    length = jnp.max(jnp.where(list_row < 0.0, 0.0, rank_row + 1.0), axis=1, keepdims=True)
    table_ref[6:7, 0:1] = length.astype(jnp.int32)


def fused_kernel(
    light,
    size,
    table_hbm,
    grads_hbm,
    left_hbm,
    right_hbm,
    settled,
    table,
    grads,
    left,
    right,
    x_out,
    x_in,
    summed,
    heavy_sum,
    ring_in,
    near_out,
    near_in,
    gradient,
    update,
    far_out,
    far_in,
    ring_out,
    heavy_result,
    back_in,
    load_sem,
    stat_sem,
    x_send,
    x_recv,
    in_send,
    in_recv,
    out_send,
    out_recv,
    ring_send,
    ring_recv,
    near_send,
    near_recv,
    back_send,
    back_recv,
    *result,
):
    levels, shards, rows, width = gradient.shape
    heavy = levels - light
    stride = stride_of(shards)
    part = shards // stride
    longest = stride * heavy
    side = light * shards + part * longest
    group, me = lax.axis_index("dp"), lax.axis_index("fsdp")
    ring, rest = me // stride, lax.rem(me, stride)
    partner = (1 - group, me)
    sequence = [2, 3, 0, 1]
    x_sequence = [*range(light, levels), *range(light)]
    place_of = {level: p for p, level in enumerate(sequence)}

    def block_at(holder, s, owner):
        return table[0, (holder * levels + s) * shards + owner]

    def block_in(holder, q, i):
        return table[2, (holder * part + q) * longest + i]

    offsets = [*range(part // 2, part), *range(1, part // 2), 0]

    def ring_at(j):
        return lax.rem(ring + offsets[j], part)

    def ring_from(j):
        return lax.rem(ring - offsets[j] + part, part)

    def visited(i):
        return ring_at(i % part) * stride + lax.rem(rest + i // part, stride)

    def remote(source, target, send, recv, device):
        return pltpu.make_async_remote_copy(
            src_ref=source,
            dst_ref=target,
            send_sem=send,
            recv_sem=recv,
            device_id=device,
            device_id_type=MESH,
        )

    loads = [
        pltpu.make_async_copy(table_hbm, table, load_sem.at[0]),
        pltpu.make_async_copy(grads_hbm, grads, load_sem.at[1]),
    ]
    for copy in loads:
        copy.start()
    barrier = pltpu.get_barrier_semaphore()
    pl.semaphore_signal(barrier, inc=1, device_id=partner, device_id_type=MESH)

    @pl.loop(1, shards)
    def _(k):
        pl.semaphore_signal(
            barrier, inc=1, device_id=(group, lax.rem(me + k, shards)), device_id_type=MESH
        )

    def stat_copies(level):
        p = place_of[level]
        return [
            pltpu.make_async_copy(left_hbm.at[level], left.at[p], stat_sem.at[0, p]),
            pltpu.make_async_copy(right_hbm.at[level], right.at[p], stat_sem.at[1, p]),
        ]

    for level in sequence:
        for copy in stat_copies(level):
            copy.start()

    packets = []
    for level in x_sequence:
        if level < light:
            for j in range(stride):
                places = range(j * part, (j + 1) * part)
                packets.append(
                    (
                        level * shards + j * part,
                        [functools.partial(block_at, s=level, owner=visited(i)) for i in places],
                    )
                )
        elif level == light:
            for q in range(part):
                packets.append(
                    (
                        light * shards + q * size,
                        [functools.partial(block_in, q=ring_at(q), i=i) for i in range(size)],
                    )
                )
    first_packet = {}
    count = 0
    for level in x_sequence:
        if level <= light:
            first_packet[level] = count
            count += stride if level < light else part

    def x_copy(n):
        start, blocks = packets[n]
        span = pl.ds(start, len(blocks))
        return remote(x_out.at[span], x_in.at[span], x_send.at[n], x_recv.at[n], partner)

    def fill(n):
        start, blocks = packets[n]
        for i, block in enumerate(blocks):
            x_out[start + i] = grads[block(1 - group)]

    for copy in loads:
        copy.wait()
    fill(0)
    pl.semaphore_wait(barrier, shards)
    for n in range(len(packets)):
        x_copy(n).start()
        if n + 1 < len(packets):
            fill(n + 1)

    def total(n, i):
        start, blocks = packets[n]
        mine = grads[blocks[i](group)].astype(jnp.float32)
        return (mine + x_in[start + i].astype(jnp.float32)).astype(jnp.bfloat16)

    def unless(condition, step):
        @pl.when(jnp.logical_not(condition))
        def _():
            step()

    def other(k):
        return lax.rem(me + k, shards)

    def in_copy(s, owner, source):
        return remote(
            summed.at[s, owner],
            gradient.at[place_of[s], source],
            in_send.at[s, owner],
            in_recv.at[s, source],
            (group, owner),
        )

    def out_copy(s, shard, source):
        spot = lax.rem(source, stride) * part + source // stride
        return remote(
            update.at[place_of[s], shard],
            result[s].at[spot],
            out_send.at[s, shard],
            out_recv.at[s, source],
            (group, shard),
        )

    def back_copy(s, j):
        from_rest = lax.rem(rest - j + stride, stride)
        span = pl.ds(from_rest * part, part)
        landing = pl.ds(s * shards + from_rest * part, part)
        n = s * stride + j
        return remote(result[s].at[span], back_in.at[landing], back_send.at[n], back_recv.at[n], partner)

    def scatter(s, first, last):
        for j in range(first, last):
            n = first_packet[s] + j
            x_copy(n).wait_recv()
            for i in range(part):
                summed[s, visited(j * part + i)] = total(n, i)
            for i in range(part):
                owner = visited(j * part + i)
                if j == 0:
                    unless(owner == me, in_copy(s, owner, me).start)
                else:
                    in_copy(s, owner, me).start()
        if first == 0:
            gradient[place_of[s], me] = summed[s, me]

    def spread(s):
        result[s][rest * part + ring] = update[place_of[s], me]
        for i in range(shards):
            if i < part:
                unless(visited(i) == me, out_copy(s, visited(i), me).start)
            else:
                out_copy(s, visited(i), me).start()

    def give_back(s):
        for j in range(stride):
            for q in range(part):
                source = q * stride + lax.rem(rest - j + stride, stride)
                if j == 0:
                    unless(source == me, out_copy(s, me, source).wait_recv)
                else:
                    out_copy(s, me, source).wait_recv()
            back_copy(s, j).start()
        for i in range(shards):
            settled[s * shards + i] = result[s][i]

    def ring_in_copy(q, source):
        return remote(
            heavy_sum.at[q],
            ring_in.at[source],
            ring_send.at[0, q],
            ring_recv.at[0, source],
            (group, q * stride + rest),
        )

    def near_in_copy(t, r, source):
        return remote(
            near_out.at[t, r],
            near_in.at[t, source],
            near_send.at[0, t, r],
            near_recv.at[0, t, source],
            (group, ring * stride + r),
        )

    def near_out_copy(t, r, source):
        return remote(
            far_out.at[t, r],
            far_in.at[t * stride + source],
            near_send.at[1, t, r],
            near_recv.at[1, t, source],
            (group, ring * stride + r),
        )

    def ring_out_copy(q, source):
        return remote(
            ring_out.at[q],
            heavy_result.at[source],
            ring_send.at[1, q],
            ring_recv.at[1, source],
            (group, q * stride + rest),
        )

    def heavy_back_copy(q):
        landing = pl.ds(light * shards + q * longest, size)
        n = light * stride + q
        return remote(heavy_result.at[q], back_in.at[landing], back_send.at[n], back_recv.at[n], partner)

    def ring_scatter(j):
        n = first_packet[light] + j
        x_copy(n).wait_recv()
        for i in range(size):
            heavy_sum[ring_at(j), i] = total(n, i)
        if offsets[j]:
            ring_in_copy(ring_at(j), ring).start()

    def near_scatter():
        ring_in[ring] = heavy_sum[ring]
        for j in range(part - 1):
            ring_in_copy(ring, ring_from(j)).wait_recv()
        for t in range(heavy):
            slot = group * levels + light + t
            for r in range(stride):
                place = table[1, slot * shards + ring * stride + r]
                for q in range(part):
                    near_out[t, r, q] = ring_in[q, place]
            for r in range(stride):
                unless(r == rest, near_in_copy(t, r, rest).start)
            near_in[t, rest] = near_out[t, rest]

    def near_spread(t):
        for r in range(stride):
            for q in range(part):
                far_out[t, r, q] = update[place_of[light + t], q * stride + r]
        for r in range(stride):
            unless(r == rest, near_out_copy(t, r, rest).start)
        far_in[t * stride + rest] = far_out[t, rest]

    def ring_spread():
        for t in range(heavy):
            for r in range(stride):
                unless(r == rest, near_out_copy(t, rest, r).wait_recv)
        for i in range(size):
            spot = table[3, (group * part + ring) * longest + i]
            for q in range(part):
                ring_out[q, i] = far_in[spot, q]
        for j in range(part - 1):
            ring_out_copy(ring_at(j), ring).start()
        heavy_result[ring] = ring_out[ring]

    def heavy_give_back():
        heavy_back_copy(ring).start()
        for j in range(part - 1):
            ring_out_copy(ring, ring_from(j)).wait_recv()
            heavy_back_copy(ring_from(j)).start()
        for q in range(part):
            for i in range(size):
                settled[light * shards + q * longest + i] = heavy_result[q, i]

    def ready(level):
        p = place_of[level]
        if level < light:

            @pl.loop(1, shards)
            def _(k):
                in_copy(level, me, other(k)).wait_recv()

        else:
            t = level - light
            for r in range(stride):
                unless(r == rest, near_in_copy(t, rest, r).wait_recv)
            for r in range(stride):
                for q in range(part):
                    gradient[p, q * stride + r] = near_in[t, r, q]
        for copy in stat_copies(level):
            copy.wait()

    def before(p):
        if p == 0:
            ring_scatter(0)
            ring_scatter(1)
            ring_scatter(2)
            ring_scatter(3)
            near_scatter()
            scatter(0, 0, 2)
        return

    def after(p):
        if p == 0:
            near_spread(0)
            scatter(0, 2, 4)
        if p == 1:
            near_spread(1)
            scatter(1, 0, 4)
        if p == 2:
            spread(0)
            ring_spread()
        if p == 3:
            spread(1)
        return

    def finish():
        give_back(0)
        heavy_give_back()
        give_back(1)

    @pl.loop(0, levels)
    def _(step):
        for p, level in enumerate(sequence):

            @pl.when(step == p)
            def _():
                before(p)
                ready(level)

        block = gradient[step].reshape(shards * rows, width)
        update[step] = shape_block(block, left[step], right[step]).reshape(shards, rows, width)
        for p, level in enumerate(sequence):

            @pl.when(step == p)
            def _():
                after(p)

    finish()
    for s in range(light):
        for j in range(stride):
            back_copy(s, j).wait_recv()
        for i in range(shards):
            settled[side + s * shards + i] = back_in[s * shards + i]
        if s == 0:
            for q in range(part):
                heavy_back_copy(q).wait_recv()
                for i in range(size):
                    spot = light * shards + q * longest + i
                    settled[side + spot] = back_in[spot]
    for s in range(light):

        @pl.loop(1, shards)
        def _(k):
            in_copy(s, other(k), me).wait_send()
            out_copy(s, other(k), me).wait_send()

        for j in range(stride):
            back_copy(s, j).wait_send()
    for q in range(part):
        heavy_back_copy(q).wait_send()
        unless(q == ring, ring_in_copy(q, ring).wait_send)
        unless(q == ring, ring_out_copy(q, ring).wait_send)
    for t in range(heavy):
        for r in range(stride):
            unless(r == rest, near_in_copy(t, r, rest).wait_send)
            unless(r == rest, near_out_copy(t, r, rest).wait_send)
    for n in range(len(packets)):
        x_copy(n).wait_send()


def settle_kernel(table, settled, out):
    member = lax.axis_index("dp")
    for b in range(out.shape[0]):
        out[b] = settled[table[4 + member, b]]


def pair_body(group_grads, owners, stats_left, stats_right):
    shards = lax.axis_size("fsdp")
    _, blocks, rows, width = group_grads.shape
    levels = stats_left.shape[1]
    caps = level_caps(blocks, shards, 2 * levels, levels)
    light = min(sum(cap == shards for cap in caps), levels - 1)
    heavy = levels - light
    stride = stride_of(shards)
    part = shards // stride
    longest = stride * heavy
    short = min(longest, -(-sum(caps[light:]) // part))
    side = light * shards + part * longest
    dma = pltpu.SemaphoreType.DMA
    bf16 = jnp.bfloat16
    vmem = pl.BlockSpec(memory_space=pltpu.VMEM)
    smem = pl.BlockSpec(memory_space=pltpu.SMEM)
    hbm = pl.BlockSpec(memory_space=pltpu.HBM)

    def pieces(*shape):
        return pltpu.VMEM((*shape, rows, width), bf16)

    table = pl.pallas_call(
        functools.partial(table_kernel, light, heavy, shards),
        out_shape=jax.ShapeDtypeStruct((8, max(2 * levels * shards, blocks)), jnp.int32),
        in_specs=[vmem],
        out_specs=vmem,
    )(owners.reshape(1, blocks))
    packets = light * stride + part

    def fused(size, number):
        return pl.pallas_call(
            functools.partial(fused_kernel, light, size),
            out_shape=jax.ShapeDtypeStruct((2 * side, rows, width), bf16),
            in_specs=[hbm] * 4,
            out_specs=vmem,
            scratch_shapes=[
                pltpu.SMEM(table.shape, jnp.int32),
                pieces(blocks),
                pltpu.VMEM((levels, width, width), jnp.float32),
                pltpu.VMEM((levels, width, width), jnp.float32),
                pieces(light * shards + part * size),
                pieces(light * shards + part * size),
                pieces(light, shards),
                pieces(part, size),
                pieces(part, size),
                pieces(heavy, stride, part),
                pieces(heavy, stride, part),
                pieces(levels, shards),
                pieces(levels, shards),
                pieces(heavy, stride, part),
                pieces(heavy * stride, part),
                pieces(part, size),
                pieces(part, size),
                pieces(side),
                dma((2,)),
                dma((2, levels)),
                dma((packets,)),
                dma((packets,)),
                dma((light, shards)),
                dma((light, shards)),
                dma((light, shards)),
                dma((light, shards)),
                dma((2, part)),
                dma((2, part)),
                dma((2, heavy, stride)),
                dma((2, heavy, stride)),
                dma((packets,)),
                dma((packets,)),
            ]
            + [pieces(shards)] * light,
            compiler_params=pltpu.CompilerParams(
                collective_id=number, has_side_effects=True, vmem_limit_bytes=48 * 1024 * 1024
            ),
        )

    settle = pl.pallas_call(
        settle_kernel,
        out_shape=jax.ShapeDtypeStruct((blocks, rows, width), bf16),
        in_specs=[smem, vmem],
        out_specs=vmem,
        compiler_params=pltpu.CompilerParams(vmem_limit_bytes=16 * 1024 * 1024),
    )

    def with_lists(size, number):
        def run(table, *arrays):
            return settle(table, fused(size, number)(table, *arrays))

        return run

    return lax.cond(
        table[6, 0] <= short,
        with_lists(short, 0),
        with_lists(longest, 1),
        table,
        group_grads[0],
        stats_left[0],
        stats_right[0],
    )


def body(group_grads, owners, stats_left, stats_right):
    groups = lax.axis_size("dp")
    member = lax.axis_index("dp")
    shards = lax.axis_size("fsdp")
    per_member = stats_left.shape[1]
    capacity = per_member * groups
    owner_of, slot_of, positions = slot_table(owners)
    local = group_grads[0]
    total = local.astype(jnp.float32)
    for step in range(1, groups):
        total = total + shifted(local, groups, step).astype(jnp.float32)
    summed = total.astype(jnp.bfloat16)
    rows_here = summed.shape[1]
    block_width = summed.shape[2]
    wanted = member * per_member + jnp.arange(per_member, dtype=jnp.int32)
    targets = (jnp.arange(shards, dtype=jnp.int32)[:, None] * capacity + wanted[None, :]).reshape(
        -1
    )
    block_key = owner_of * capacity + slot_of
    matches = targets[:, None] == block_key[None, :]
    present = jnp.any(matches, axis=1)
    chosen = jnp.sum(jnp.where(matches, positions[None, :], 0), axis=1)
    outgoing = jnp.where(
        present[:, None, None], jnp.take(summed, chosen, axis=0), jnp.zeros((), jnp.bfloat16)
    )
    outgoing = outgoing.reshape(shards, per_member, rows_here, block_width)
    arrived = lax.all_to_all(outgoing, "fsdp", split_axis=0, concat_axis=2, tiled=True)
    gradient = arrived.reshape(per_member, block_width, block_width)
    update = shape_blocks(gradient, stats_left[0], stats_right[0])
    pieces = update.reshape(per_member, shards, rows_here, block_width)
    returned = lax.all_to_all(pieces, "fsdp", split_axis=1, concat_axis=0, tiled=True)
    returned = returned.reshape(shards * per_member, rows_here, block_width)
    mine = jnp.take(returned, owner_of * per_member + slot_of % per_member, axis=0)
    holder = slot_of // per_member
    result = mine
    for step in range(1, groups):
        theirs = (holder == (member - step) % groups)[:, None, None]
        result = jnp.where(theirs, shifted(mine, groups, step), result)
    return result


def solution(mesh):
    placed = (
        P("dp", None, "fsdp", None),
        P(),
        P("fsdp", "dp", None, None),
        P("fsdp", "dp", None, None),
    )
    return jax.shard_map(
        pair_body if mesh.shape["dp"] == 2 else body, mesh=mesh, in_specs=placed, out_specs=P(None, "fsdp", None), check_vma=False
    )
```

```python
import functools
import math
import jax
import jax.numpy as jnp
from jax import lax
from jax.experimental import pallas as pl
from jax.experimental.pallas import tpu as pltpu
from jax.sharding import PartitionSpec as P

ITERS = 2


BETA = 0.95

POWER = [math.comb(5, j) * 5.0 ** (5 - j) * (-1.0) ** j / 4.0**6 for j in range(6)]
COEF = [25.0 / 16.0, -5.0 / 16.0 - POWER[0]] + [-POWER[j] for j in range(1, 6)]


def mm(former, latter, dims=((1,), (0,))):
    return lax.dot_general(former, latter, (dims, ((), ())), preferred_element_type=jnp.float32)


def total_of(value):
    return jnp.sum(jnp.sum(value, axis=0, keepdims=True), axis=1, keepdims=True)


def newton_root(statistic):
    magnitude = jnp.sqrt(total_of(statistic * statistic) + 1e-06)
    first = statistic * (1.0 / magnitude)
    low_first = first.astype(jnp.bfloat16)
    second = mm(low_first, low_first)
    third = mm(second.astype(jnp.bfloat16), low_first)
    upper = COEF[4] * first + COEF[5] * second + COEF[6] * third
    lower = COEF[1] * first + COEF[2] * second + COEF[3] * third
    factor = lower + mm(third.astype(jnp.bfloat16), upper.astype(jnp.bfloat16))
    row = lax.broadcasted_iota(jnp.int32, factor.shape, 0)
    column = lax.broadcasted_iota(jnp.int32, factor.shape, 1)
    return (factor + jnp.where(row == column, COEF[0], 0.0)).astype(jnp.bfloat16)


def shape_kernel(gradient_ref, left_ref, right_ref, update_ref):
    gradient = gradient_ref[0]
    left_root = newton_root(BETA * left_ref[0] + mm(gradient, gradient, ((1,), (1,))))
    halfway = mm(left_root, gradient).astype(jnp.bfloat16)
    right_root = newton_root(BETA * right_ref[0] + mm(gradient, gradient, ((0,), (0,))))
    shaped = mm(halfway, right_root)
    wide = gradient.astype(jnp.float32)
    ratio = jnp.sqrt(total_of(wide * wide)) / jnp.sqrt(total_of(shaped * shaped) + 1e-06)
    update_ref[0] = (shaped * ratio).astype(jnp.bfloat16)


def shape_blocks(gradient, left, right, interpret=False):
    count, width, _ = gradient.shape
    spec = pl.BlockSpec((1, width, width), lambda k: (k, 0, 0))
    return pl.pallas_call(
        shape_kernel,
        grid=(count,),
        out_shape=jax.ShapeDtypeStruct(gradient.shape, jnp.bfloat16),
        in_specs=[spec] * 3,
        out_specs=spec,
        compiler_params=pltpu.CompilerParams(vmem_limit_bytes=48 * 1024 * 1024),
        cost_estimate=pl.CostEstimate(
            flops=20 * count * width**3, bytes_accessed=12 * count * width**2, transcendentals=0
        ),
        interpret=interpret,
    )(gradient, left, right)


def shifted(value, groups, step):
    return lax.ppermute(value, "dp", [(g, (g + step) % groups) for g in range(groups)])


def slot_table(owners):
    owner_of = owners[:, 0]
    positions = jnp.arange(owner_of.shape[0], dtype=jnp.int32)
    earlier = (owner_of[None, :] == owner_of[:, None]) & (positions[None, :] < positions[:, None])
    slot_of = jnp.sum(earlier.astype(jnp.int32), axis=1)
    return (owner_of, slot_of, positions)

MESH = pl.DeviceIdType.MESH


def shape_block(gradient, left, right):
    left_root = newton_root(BETA * left + mm(gradient, gradient, ((1,), (1,))))
    halfway = mm(left_root, gradient).astype(jnp.bfloat16)
    right_root = newton_root(BETA * right + mm(gradient, gradient, ((0,), (0,))))
    shaped = mm(halfway, right_root)
    wide = gradient.astype(jnp.float32)
    ratio = jnp.sqrt(total_of(wide * wide)) / jnp.sqrt(total_of(shaped * shaped) + 1e-06)
    return (shaped * ratio).astype(jnp.bfloat16)


def level_caps(blocks, shards, capacity, levels):
    caps = [shards]
    for slot in range(1, levels):
        caps.append(min(shards, (blocks - capacity + slot + 1 - shards) // slot))
    return caps


def stride_of(shards):
    return next(s for s in range(math.isqrt(shards), 0, -1) if shards % s == 0)


def table_kernel(light, heavy, shards, owners_ref, table_ref):
    blocks = owners_ref.shape[1]
    levels = light + heavy
    stride = stride_of(shards)
    part = shards // stride
    longest = stride * heavy

    def numbers(shape, axis):
        return lax.broadcasted_iota(jnp.int32, shape, axis).astype(jnp.float32)

    def split(value, size):
        quotient = jnp.floor((value + 0.5) * (1.0 / size))
        return quotient, value - size * quotient

    def down(mask, value=1.0):
        return jnp.sum(jnp.where(mask, value, 0.0), axis=0, keepdims=True)

    def across(mask, value=1.0):
        return jnp.sum(jnp.where(mask, value, 0.0), axis=1, keepdims=True)

    def listed(owner, slot):
        holder, depth = split(slot, levels)
        ring, rest = split(owner, stride)
        name = jnp.where(depth >= light, holder * part + ring, -1.0)
        return name, depth * stride + rest

    square = (blocks, blocks)
    first, second = numbers(square, 0), numbers(square, 1)
    owner_row = owners_ref[...].astype(jnp.float32)
    owner_col = across(first == second, owner_row)
    same = owner_col == owner_row
    slot_row = down(same & (first < second))
    slot_col = across(same & (second < first))
    list_row, key_row = listed(owner_row, slot_row)
    list_col, key_col = listed(owner_col, slot_col)
    together = list_col == list_row
    rank_row = down(together & (key_col < key_row))
    rank_col = across(together & (key_row < key_col))
    wide = (blocks, 2 * levels * shards)
    slot, owner = split(numbers(wide, 1), shards)
    at_owner = (slot_col == slot) & (owner_col == owner)
    block_col = numbers(wide, 0)
    lists = (blocks, 2 * part * longest)
    name, place = split(numbers(lists, 1), longest)
    at_place = (list_col == name) & (rank_col == place)
    rows = [
        down(at_owner, block_col),
        down(at_owner & (list_col >= 0.0), rank_col),
        down(at_place, numbers(lists, 0)),
        down(at_place, key_col - light * stride),
    ]
    for r, row in enumerate(rows):
        table_ref[r : r + 1, 0 : row.shape[1]] = row.astype(jnp.int32)
    holder, depth = split(slot_row, levels)
    ring, rest = split(owner_row, stride)
    near = jnp.where(
        list_row < 0.0,
        depth * shards + rest * part + ring,
        light * shards + ring * longest + rank_row,
    )
    side = light * shards + part * longest
    for member in range(2):
        pick = near + jnp.where(holder == member, 0.0, float(side))
        table_ref[4 + member : 5 + member, 0:blocks] = pick.astype(jnp.int32)
    length = jnp.max(jnp.where(list_row < 0.0, 0.0, rank_row + 1.0), axis=1, keepdims=True)
    table_ref[6:7, 0:1] = length.astype(jnp.int32)


def fused_kernel(
    light,
    size,
    table_hbm,
    grads_hbm,
    left_hbm,
    right_hbm,
    settled,
    table,
    grads,
    left,
    right,
    x_out,
    x_in,
    summed,
    heavy_sum,
    ring_in,
    near_out,
    near_in,
    gradient,
    update,
    far_out,
    far_in,
    ring_out,
    heavy_result,
    back_in,
    load_sem,
    stat_sem,
    x_send,
    x_recv,
    in_send,
    in_recv,
    out_send,
    out_recv,
    ring_send,
    ring_recv,
    near_send,
    near_recv,
    back_send,
    back_recv,
    *result,
):
    levels, shards, rows, width = gradient.shape
    heavy = levels - light
    stride = stride_of(shards)
    part = shards // stride
    longest = stride * heavy
    side = light * shards + part * longest
    group, me = lax.axis_index("dp"), lax.axis_index("fsdp")
    ring, rest = me // stride, lax.rem(me, stride)
    partner = (1 - group, me)
    sequence = [*range(light, levels), *range(light)]
    place_of = {level: p for p, level in enumerate(sequence)}

    def block_at(holder, s, owner):
        return table[0, (holder * levels + s) * shards + owner]

    def block_in(holder, q, i):
        return table[2, (holder * part + q) * longest + i]

    offsets = [*range(part // 2, part), *range(1, part // 2), 0]

    def ring_at(j):
        return lax.rem(ring + offsets[j], part)

    def ring_from(j):
        return lax.rem(ring - offsets[j] + part, part)

    def visited(i):
        return ring_at(i % part) * stride + lax.rem(rest + i // part, stride)

    def remote(source, target, send, recv, device):
        return pltpu.make_async_remote_copy(
            src_ref=source,
            dst_ref=target,
            send_sem=send,
            recv_sem=recv,
            device_id=device,
            device_id_type=MESH,
        )

    loads = [
        pltpu.make_async_copy(table_hbm, table, load_sem.at[0]),
        pltpu.make_async_copy(grads_hbm, grads, load_sem.at[1]),
    ]
    for copy in loads:
        copy.start()
    barrier = pltpu.get_barrier_semaphore()
    pl.semaphore_signal(barrier, inc=1, device_id=partner, device_id_type=MESH)

    @pl.loop(1, shards)
    def _(k):
        pl.semaphore_signal(
            barrier, inc=1, device_id=(group, lax.rem(me + k, shards)), device_id_type=MESH
        )

    def stat_copies(level):
        p = place_of[level]
        return [
            pltpu.make_async_copy(left_hbm.at[level], left.at[p], stat_sem.at[0, p]),
            pltpu.make_async_copy(right_hbm.at[level], right.at[p], stat_sem.at[1, p]),
        ]

    for level in sequence:
        for copy in stat_copies(level):
            copy.start()

    packets = []
    for level in sequence:
        if level < light:
            for j in range(stride):
                places = range(j * part, (j + 1) * part)
                packets.append(
                    (
                        level * shards + j * part,
                        [functools.partial(block_at, s=level, owner=visited(i)) for i in places],
                    )
                )
        elif level == light:
            for q in range(part):
                packets.append(
                    (
                        light * shards + q * size,
                        [functools.partial(block_in, q=ring_at(q), i=i) for i in range(size)],
                    )
                )
    first_packet = {}
    count = 0
    for level in sequence:
        if level <= light:
            first_packet[level] = count
            count += stride if level < light else part

    def x_copy(n):
        start, blocks = packets[n]
        span = pl.ds(start, len(blocks))
        return remote(x_out.at[span], x_in.at[span], x_send.at[n], x_recv.at[n], partner)

    def fill(n):
        start, blocks = packets[n]
        for i, block in enumerate(blocks):
            x_out[start + i] = grads[block(1 - group)]

    for copy in loads:
        copy.wait()
    fill(0)
    pl.semaphore_wait(barrier, shards)
    for n in range(len(packets)):
        x_copy(n).start()
        if n + 1 < len(packets):
            fill(n + 1)

    def total(n, i):
        start, blocks = packets[n]
        mine = grads[blocks[i](group)].astype(jnp.float32)
        return (mine + x_in[start + i].astype(jnp.float32)).astype(jnp.bfloat16)

    def unless(condition, step):
        @pl.when(jnp.logical_not(condition))
        def _():
            step()

    def other(k):
        return lax.rem(me + k, shards)

    def in_copy(s, owner, source):
        return remote(
            summed.at[s, owner],
            gradient.at[place_of[s], source],
            in_send.at[s, owner],
            in_recv.at[s, source],
            (group, owner),
        )

    def out_copy(s, shard, source):
        spot = lax.rem(source, stride) * part + source // stride
        return remote(
            update.at[place_of[s], shard],
            result[s].at[spot],
            out_send.at[s, shard],
            out_recv.at[s, source],
            (group, shard),
        )

    def back_copy(s, j):
        from_rest = lax.rem(rest - j + stride, stride)
        span = pl.ds(from_rest * part, part)
        landing = pl.ds(s * shards + from_rest * part, part)
        n = s * stride + j
        return remote(result[s].at[span], back_in.at[landing], back_send.at[n], back_recv.at[n], partner)

    def scatter(s, first, last):
        for j in range(first, last):
            n = first_packet[s] + j
            x_copy(n).wait_recv()
            for i in range(part):
                summed[s, visited(j * part + i)] = total(n, i)
            for i in range(part):
                owner = visited(j * part + i)
                if j == 0:
                    unless(owner == me, in_copy(s, owner, me).start)
                else:
                    in_copy(s, owner, me).start()
        if first == 0:
            gradient[place_of[s], me] = summed[s, me]

    def spread(s):
        result[s][rest * part + ring] = update[place_of[s], me]
        for i in range(shards):
            if i < part:
                unless(visited(i) == me, out_copy(s, visited(i), me).start)
            else:
                out_copy(s, visited(i), me).start()

    def give_back(s):
        for j in range(stride):
            for q in range(part):
                source = q * stride + lax.rem(rest - j + stride, stride)
                if j == 0:
                    unless(source == me, out_copy(s, me, source).wait_recv)
                else:
                    out_copy(s, me, source).wait_recv()
            back_copy(s, j).start()
        for i in range(shards):
            settled[s * shards + i] = result[s][i]

    def ring_in_copy(q, source):
        return remote(
            heavy_sum.at[q],
            ring_in.at[source],
            ring_send.at[0, q],
            ring_recv.at[0, source],
            (group, q * stride + rest),
        )

    def near_in_copy(t, r, source):
        return remote(
            near_out.at[t, r],
            near_in.at[t, source],
            near_send.at[0, t, r],
            near_recv.at[0, t, source],
            (group, ring * stride + r),
        )

    def near_out_copy(t, r, source):
        return remote(
            far_out.at[t, r],
            far_in.at[t * stride + source],
            near_send.at[1, t, r],
            near_recv.at[1, t, source],
            (group, ring * stride + r),
        )

    def ring_out_copy(q, source):
        return remote(
            ring_out.at[q],
            heavy_result.at[source],
            ring_send.at[1, q],
            ring_recv.at[1, source],
            (group, q * stride + rest),
        )

    def heavy_back_copy(q):
        landing = pl.ds(light * shards + q * longest, size)
        n = light * stride + q
        return remote(heavy_result.at[q], back_in.at[landing], back_send.at[n], back_recv.at[n], partner)

    def ring_scatter(j):
        n = first_packet[light] + j
        x_copy(n).wait_recv()
        for i in range(size):
            heavy_sum[ring_at(j), i] = total(n, i)
        if offsets[j]:
            ring_in_copy(ring_at(j), ring).start()

    def near_scatter():
        ring_in[ring] = heavy_sum[ring]
        for j in range(part - 1):
            ring_in_copy(ring, ring_from(j)).wait_recv()
        for t in range(heavy):
            slot = group * levels + light + t
            for r in range(stride):
                place = table[1, slot * shards + ring * stride + r]
                for q in range(part):
                    near_out[t, r, q] = ring_in[q, place]
            for r in range(stride):
                unless(r == rest, near_in_copy(t, r, rest).start)
            near_in[t, rest] = near_out[t, rest]

    def near_spread(t):
        for r in range(stride):
            for q in range(part):
                far_out[t, r, q] = update[place_of[light + t], q * stride + r]
        for r in range(stride):
            unless(r == rest, near_out_copy(t, r, rest).start)
        far_in[t * stride + rest] = far_out[t, rest]

    def ring_spread():
        for t in range(heavy):
            for r in range(stride):
                unless(r == rest, near_out_copy(t, rest, r).wait_recv)
        for i in range(size):
            spot = table[3, (group * part + ring) * longest + i]
            for q in range(part):
                ring_out[q, i] = far_in[spot, q]
        for j in range(part - 1):
            ring_out_copy(ring_at(j), ring).start()
        heavy_result[ring] = ring_out[ring]

    def heavy_give_back():
        heavy_back_copy(ring).start()
        for j in range(part - 1):
            ring_out_copy(ring, ring_from(j)).wait_recv()
            heavy_back_copy(ring_from(j)).start()
        for q in range(part):
            for i in range(size):
                settled[light * shards + q * longest + i] = heavy_result[q, i]

    def ready(level):
        p = place_of[level]
        if level < light:

            @pl.loop(1, shards)
            def _(k):
                in_copy(level, me, other(k)).wait_recv()

        else:
            t = level - light
            for r in range(stride):
                unless(r == rest, near_in_copy(t, rest, r).wait_recv)
            for r in range(stride):
                for q in range(part):
                    gradient[p, q * stride + r] = near_in[t, r, q]
        for copy in stat_copies(level):
            copy.wait()

    half = stride // 2

    def before(p):
        if p == 0:
            for j in range(part):
                ring_scatter(j)
            near_scatter()
            scatter(0, 0, half)

    def after(p):
        if p < heavy:
            near_spread(p)
            if p == 0:
                scatter(0, half, stride)
            if p == heavy - 1:
                for s in range(1, light):
                    scatter(s, 0, stride)
        else:
            spread(p - heavy)
            if p == heavy:
                ring_spread()

    @pl.loop(0, levels)
    def _(step):
        for p, level in enumerate(sequence):

            @pl.when(step == p)
            def _():
                before(p)
                ready(level)

        block = gradient[step].reshape(shards * rows, width)
        update[step] = shape_block(block, left[step], right[step]).reshape(shards, rows, width)
        for p, level in enumerate(sequence):

            @pl.when(step == p)
            def _():
                after(p)

    give_back(0)
    heavy_give_back()
    for s in range(1, light):
        give_back(s)
    for s in range(light):
        for j in range(stride):
            back_copy(s, j).wait_recv()
        for i in range(shards):
            settled[side + s * shards + i] = back_in[s * shards + i]
        if s == 0:
            for q in range(part):
                heavy_back_copy(q).wait_recv()
                for i in range(size):
                    spot = light * shards + q * longest + i
                    settled[side + spot] = back_in[spot]
    for s in range(light):

        @pl.loop(1, shards)
        def _(k):
            in_copy(s, other(k), me).wait_send()
            out_copy(s, other(k), me).wait_send()

        for j in range(stride):
            back_copy(s, j).wait_send()
    for q in range(part):
        heavy_back_copy(q).wait_send()
        unless(q == ring, ring_in_copy(q, ring).wait_send)
        unless(q == ring, ring_out_copy(q, ring).wait_send)
    for t in range(heavy):
        for r in range(stride):
            unless(r == rest, near_in_copy(t, r, rest).wait_send)
            unless(r == rest, near_out_copy(t, r, rest).wait_send)
    for n in range(len(packets)):
        x_copy(n).wait_send()


def settle_kernel(table, settled, out):
    member = lax.axis_index("dp")
    for b in range(out.shape[0]):
        out[b] = settled[table[4 + member, b]]


def pair_body(group_grads, owners, stats_left, stats_right):
    shards = lax.axis_size("fsdp")
    _, blocks, rows, width = group_grads.shape
    levels = stats_left.shape[1]
    if levels == 1:
        return body(group_grads, owners, stats_left, stats_right)
    caps = level_caps(blocks, shards, 2 * levels, levels)
    light = min(sum(cap == shards for cap in caps), levels - 1)
    heavy = levels - light
    stride = stride_of(shards)
    part = shards // stride
    longest = stride * heavy
    fair = -(-sum(caps[light:]) // part)
    sizes = [size for size in range(max(1, fair - 2), fair + 1) if size < longest] + [longest]
    side = light * shards + part * longest
    dma = pltpu.SemaphoreType.DMA
    bf16 = jnp.bfloat16
    vmem = pl.BlockSpec(memory_space=pltpu.VMEM)
    smem = pl.BlockSpec(memory_space=pltpu.SMEM)
    hbm = pl.BlockSpec(memory_space=pltpu.HBM)

    def pieces(*shape):
        return pltpu.VMEM((*shape, rows, width), bf16)

    table = pl.pallas_call(
        functools.partial(table_kernel, light, heavy, shards),
        out_shape=jax.ShapeDtypeStruct((8, max(2 * levels * shards, blocks)), jnp.int32),
        in_specs=[vmem],
        out_specs=vmem,
    )(owners.reshape(1, blocks))
    packets = light * stride + part

    def fused(size, number):
        return pl.pallas_call(
            functools.partial(fused_kernel, light, size),
            out_shape=jax.ShapeDtypeStruct((2 * side, rows, width), bf16),
            in_specs=[hbm] * 4,
            out_specs=vmem,
            scratch_shapes=[
                pltpu.SMEM(table.shape, jnp.int32),
                pieces(blocks),
                pltpu.VMEM((levels, width, width), jnp.float32),
                pltpu.VMEM((levels, width, width), jnp.float32),
                pieces(light * shards + part * size),
                pieces(light * shards + part * size),
                pieces(light, shards),
                pieces(part, size),
                pieces(part, size),
                pieces(heavy, stride, part),
                pieces(heavy, stride, part),
                pieces(levels, shards),
                pieces(levels, shards),
                pieces(heavy, stride, part),
                pieces(heavy * stride, part),
                pieces(part, size),
                pieces(part, size),
                pieces(side),
                dma((2,)),
                dma((2, levels)),
                dma((packets,)),
                dma((packets,)),
                dma((light, shards)),
                dma((light, shards)),
                dma((light, shards)),
                dma((light, shards)),
                dma((2, part)),
                dma((2, part)),
                dma((2, heavy, stride)),
                dma((2, heavy, stride)),
                dma((packets,)),
                dma((packets,)),
            ]
            + [pieces(shards)] * light,
            compiler_params=pltpu.CompilerParams(
                collective_id=number, has_side_effects=True, vmem_limit_bytes=48 * 1024 * 1024
            ),
        )

    settle = pl.pallas_call(
        settle_kernel,
        out_shape=jax.ShapeDtypeStruct((blocks, rows, width), bf16),
        in_specs=[smem, vmem],
        out_specs=vmem,
        compiler_params=pltpu.CompilerParams(vmem_limit_bytes=16 * 1024 * 1024),
    )

    def with_lists(size, number):
        def run(table, *arrays):
            return settle(table, fused(size, number)(table, *arrays))

        return run

    length = table[6, 0]
    branch = sum((length > size).astype(jnp.int32) for size in sizes[:-1])
    return lax.switch(
        branch,
        [with_lists(size, number) for number, size in enumerate(sizes)],
        table,
        group_grads[0],
        stats_left[0],
        stats_right[0],
    )


def body(group_grads, owners, stats_left, stats_right):
    groups = lax.axis_size("dp")
    member = lax.axis_index("dp")
    shards = lax.axis_size("fsdp")
    per_member = stats_left.shape[1]
    capacity = per_member * groups
    owner_of, slot_of, positions = slot_table(owners)
    local = group_grads[0]
    total = local.astype(jnp.float32)
    for step in range(1, groups):
        total = total + shifted(local, groups, step).astype(jnp.float32)
    summed = total.astype(jnp.bfloat16)
    rows_here = summed.shape[1]
    block_width = summed.shape[2]
    wanted = member * per_member + jnp.arange(per_member, dtype=jnp.int32)
    targets = (jnp.arange(shards, dtype=jnp.int32)[:, None] * capacity + wanted[None, :]).reshape(
        -1
    )
    block_key = owner_of * capacity + slot_of
    matches = targets[:, None] == block_key[None, :]
    present = jnp.any(matches, axis=1)
    chosen = jnp.sum(jnp.where(matches, positions[None, :], 0), axis=1)
    outgoing = jnp.where(
        present[:, None, None], jnp.take(summed, chosen, axis=0), jnp.zeros((), jnp.bfloat16)
    )
    outgoing = outgoing.reshape(shards, per_member, rows_here, block_width)
    arrived = lax.all_to_all(outgoing, "fsdp", split_axis=0, concat_axis=2, tiled=True)
    gradient = arrived.reshape(per_member, block_width, block_width)
    update = shape_blocks(gradient, stats_left[0], stats_right[0])
    pieces = update.reshape(per_member, shards, rows_here, block_width)
    returned = lax.all_to_all(pieces, "fsdp", split_axis=1, concat_axis=0, tiled=True)
    returned = returned.reshape(shards * per_member, rows_here, block_width)
    mine = jnp.take(returned, owner_of * per_member + slot_of % per_member, axis=0)
    holder = slot_of // per_member
    result = mine
    for step in range(1, groups):
        theirs = (holder == (member - step) % groups)[:, None, None]
        result = jnp.where(theirs, shifted(mine, groups, step), result)
    return result


def solution(mesh):
    placed = (
        P("dp", None, "fsdp", None),
        P(),
        P("fsdp", "dp", None, None),
        P("fsdp", "dp", None, None),
    )
    return jax.shard_map(
        pair_body if mesh.shape["dp"] == 2 else body, mesh=mesh, in_specs=placed, out_specs=P(None, "fsdp", None), check_vma=False
    )
```

```python
import functools
import math
import jax
import jax.numpy as jnp
from jax import lax
from jax.experimental import pallas as pl
from jax.experimental.pallas import tpu as pltpu
from jax.sharding import PartitionSpec as P

ITERS = 2


BETA = 0.95

POWER = [math.comb(5, j) * 5.0 ** (5 - j) * (-1.0) ** j / 4.0**6 for j in range(6)]
COEF = [25.0 / 16.0, -5.0 / 16.0 - POWER[0]] + [-POWER[j] for j in range(1, 6)]


def mm(former, latter, dims=((1,), (0,))):
    return lax.dot_general(former, latter, (dims, ((), ())), preferred_element_type=jnp.float32)


def total_of(value):
    return jnp.sum(jnp.sum(value, axis=0, keepdims=True), axis=1, keepdims=True)


def newton_root(statistic):
    magnitude = jnp.sqrt(total_of(statistic * statistic) + 1e-06)
    first = statistic * (1.0 / magnitude)
    low_first = first.astype(jnp.bfloat16)
    second = mm(low_first, low_first)
    third = mm(second.astype(jnp.bfloat16), low_first)
    upper = COEF[4] * first + COEF[5] * second + COEF[6] * third
    lower = COEF[1] * first + COEF[2] * second + COEF[3] * third
    factor = lower + mm(third.astype(jnp.bfloat16), upper.astype(jnp.bfloat16))
    row = lax.broadcasted_iota(jnp.int32, factor.shape, 0)
    column = lax.broadcasted_iota(jnp.int32, factor.shape, 1)
    return (factor + jnp.where(row == column, COEF[0], 0.0)).astype(jnp.bfloat16)


def shape_kernel(gradient_ref, left_ref, right_ref, update_ref):
    gradient = gradient_ref[0]
    left_root = newton_root(BETA * left_ref[0] + mm(gradient, gradient, ((1,), (1,))))
    halfway = mm(left_root, gradient).astype(jnp.bfloat16)
    right_root = newton_root(BETA * right_ref[0] + mm(gradient, gradient, ((0,), (0,))))
    shaped = mm(halfway, right_root)
    wide = gradient.astype(jnp.float32)
    ratio = jnp.sqrt(total_of(wide * wide)) / jnp.sqrt(total_of(shaped * shaped) + 1e-06)
    update_ref[0] = (shaped * ratio).astype(jnp.bfloat16)


def shape_blocks(gradient, left, right, interpret=False):
    count, width, _ = gradient.shape
    spec = pl.BlockSpec((1, width, width), lambda k: (k, 0, 0))
    return pl.pallas_call(
        shape_kernel,
        grid=(count,),
        out_shape=jax.ShapeDtypeStruct(gradient.shape, jnp.bfloat16),
        in_specs=[spec] * 3,
        out_specs=spec,
        compiler_params=pltpu.CompilerParams(vmem_limit_bytes=48 * 1024 * 1024),
        cost_estimate=pl.CostEstimate(
            flops=20 * count * width**3, bytes_accessed=12 * count * width**2, transcendentals=0
        ),
        interpret=interpret,
    )(gradient, left, right)


def shifted(value, groups, step):
    return lax.ppermute(value, "dp", [(g, (g + step) % groups) for g in range(groups)])


def slot_table(owners):
    owner_of = owners[:, 0]
    positions = jnp.arange(owner_of.shape[0], dtype=jnp.int32)
    earlier = (owner_of[None, :] == owner_of[:, None]) & (positions[None, :] < positions[:, None])
    slot_of = jnp.sum(earlier.astype(jnp.int32), axis=1)
    return (owner_of, slot_of, positions)

MESH = pl.DeviceIdType.MESH


def shape_block(gradient, left, right):
    left_root = newton_root(BETA * left + mm(gradient, gradient, ((1,), (1,))))
    halfway = mm(left_root, gradient).astype(jnp.bfloat16)
    right_root = newton_root(BETA * right + mm(gradient, gradient, ((0,), (0,))))
    shaped = mm(halfway, right_root)
    wide = gradient.astype(jnp.float32)
    ratio = jnp.sqrt(total_of(wide * wide)) / jnp.sqrt(total_of(shaped * shaped) + 1e-06)
    return (shaped * ratio).astype(jnp.bfloat16)


def level_caps(blocks, shards, capacity, levels):
    caps = [shards]
    for slot in range(1, levels):
        caps.append(min(shards, (blocks - capacity + slot + 1 - shards) // slot))
    return caps


def stride_of(shards):
    return next(s for s in range(math.isqrt(shards), 0, -1) if shards % s == 0)


def table_kernel(light, heavy, shards, owners_ref, table_ref):
    blocks = owners_ref.shape[1]
    levels = light + heavy
    stride = stride_of(shards)
    part = shards // stride
    longest = stride * heavy

    def numbers(shape, axis):
        return lax.broadcasted_iota(jnp.int32, shape, axis).astype(jnp.float32)

    def split(value, size):
        quotient = jnp.floor((value + 0.5) * (1.0 / size))
        return quotient, value - size * quotient

    def down(mask, value=1.0):
        return jnp.sum(jnp.where(mask, value, 0.0), axis=0, keepdims=True)

    def across(mask, value=1.0):
        return jnp.sum(jnp.where(mask, value, 0.0), axis=1, keepdims=True)

    def listed(owner, slot):
        holder, depth = split(slot, levels)
        ring, rest = split(owner, stride)
        name = jnp.where(depth >= light, holder * part + ring, -1.0)
        return name, depth * stride + rest

    square = (blocks, blocks)
    first, second = numbers(square, 0), numbers(square, 1)
    owner_row = owners_ref[...].astype(jnp.float32)
    owner_col = across(first == second, owner_row)
    same = owner_col == owner_row
    slot_row = down(same & (first < second))
    slot_col = across(same & (second < first))
    list_row, key_row = listed(owner_row, slot_row)
    list_col, key_col = listed(owner_col, slot_col)
    together = list_col == list_row
    rank_row = down(together & (key_col < key_row))
    rank_col = across(together & (key_row < key_col))
    wide = (blocks, 2 * levels * shards)
    slot, owner = split(numbers(wide, 1), shards)
    at_owner = (slot_col == slot) & (owner_col == owner)
    block_col = numbers(wide, 0)
    lists = (blocks, 2 * part * longest)
    name, place = split(numbers(lists, 1), longest)
    at_place = (list_col == name) & (rank_col == place)
    rows = [
        down(at_owner, block_col),
        down(at_owner & (list_col >= 0.0), rank_col),
        down(at_place, numbers(lists, 0)),
        down(at_place, key_col - light * stride),
    ]
    for r, row in enumerate(rows):
        table_ref[r : r + 1, 0 : row.shape[1]] = row.astype(jnp.int32)
    holder, depth = split(slot_row, levels)
    ring, rest = split(owner_row, stride)
    near = jnp.where(
        list_row < 0.0,
        depth * shards + rest * part + ring,
        light * shards + ring * longest + rank_row,
    )
    side = light * shards + part * longest
    for member in range(2):
        pick = near + jnp.where(holder == member, 0.0, float(side))
        table_ref[4 + member : 5 + member, 0:blocks] = pick.astype(jnp.int32)
    length = jnp.max(jnp.where(list_row < 0.0, 0.0, rank_row + 1.0), axis=1, keepdims=True)
    table_ref[6:7, 0:1] = length.astype(jnp.int32)


def fused_kernel(
    light,
    size,
    table_hbm,
    grads_hbm,
    left_hbm,
    right_hbm,
    settled,
    table,
    grads,
    left,
    right,
    x_out,
    x_in,
    summed,
    heavy_sum,
    ring_in,
    near_out,
    near_in,
    gradient,
    update,
    far_out,
    far_in,
    ring_out,
    heavy_result,
    back_in,
    load_sem,
    stat_sem,
    x_send,
    x_recv,
    in_send,
    in_recv,
    out_send,
    out_recv,
    ring_send,
    ring_recv,
    near_send,
    near_recv,
    back_send,
    back_recv,
    *result,
):
    levels, shards, rows, width = gradient.shape
    heavy = levels - light
    stride = stride_of(shards)
    part = shards // stride
    longest = stride * heavy
    side = light * shards + part * longest
    group, me = lax.axis_index("dp"), lax.axis_index("fsdp")
    ring, rest = me // stride, lax.rem(me, stride)
    partner = (1 - group, me)
    sequence = [*range(light, levels), *range(light)]
    place_of = {level: p for p, level in enumerate(sequence)}

    def block_at(holder, s, owner):
        return table[0, (holder * levels + s) * shards + owner]

    def block_in(holder, q, i):
        return table[2, (holder * part + q) * longest + i]

    offsets = [*range(part // 2, part), *range(1, part // 2), 0]

    def ring_at(j):
        return lax.rem(ring + offsets[j], part)

    def ring_from(j):
        return lax.rem(ring - offsets[j] + part, part)

    def visited(i):
        return ring_at(i % part) * stride + lax.rem(rest + i // part, stride)

    def remote(source, target, send, recv, device):
        return pltpu.make_async_remote_copy(
            src_ref=source,
            dst_ref=target,
            send_sem=send,
            recv_sem=recv,
            device_id=device,
            device_id_type=MESH,
        )

    loads = [
        pltpu.make_async_copy(table_hbm, table, load_sem.at[0]),
        pltpu.make_async_copy(grads_hbm, grads, load_sem.at[1]),
    ]
    for copy in loads:
        copy.start()
    barrier = pltpu.get_barrier_semaphore()
    pl.semaphore_signal(barrier, inc=1, device_id=partner, device_id_type=MESH)

    @pl.loop(1, shards)
    def _(k):
        pl.semaphore_signal(
            barrier, inc=1, device_id=(group, lax.rem(me + k, shards)), device_id_type=MESH
        )

    def stat_copies(level):
        p = place_of[level]
        return [
            pltpu.make_async_copy(left_hbm.at[level], left.at[p], stat_sem.at[0, p]),
            pltpu.make_async_copy(right_hbm.at[level], right.at[p], stat_sem.at[1, p]),
        ]

    for level in sequence:
        for copy in stat_copies(level):
            copy.start()

    packets = []
    for level in sequence:
        if level < light:
            for j in range(stride):
                places = range(j * part, (j + 1) * part)
                packets.append(
                    (
                        level * shards + j * part,
                        [functools.partial(block_at, s=level, owner=visited(i)) for i in places],
                    )
                )
        elif level == light:
            for q in range(part):
                packets.append(
                    (
                        light * shards + q * size,
                        [functools.partial(block_in, q=ring_at(q), i=i) for i in range(size)],
                    )
                )
    first_packet = {}
    count = 0
    for level in sequence:
        if level <= light:
            first_packet[level] = count
            count += stride if level < light else part

    def x_copy(n):
        start, blocks = packets[n]
        span = pl.ds(start, len(blocks))
        return remote(x_out.at[span], x_in.at[span], x_send.at[n], x_recv.at[n], partner)

    def fill(n):
        start, blocks = packets[n]
        for i, block in enumerate(blocks):
            x_out[start + i] = grads[block(1 - group)]

    for copy in loads:
        copy.wait()
    fill(0)
    pl.semaphore_wait(barrier, shards)
    for n in range(len(packets)):
        x_copy(n).start()
        if n + 1 < len(packets):
            fill(n + 1)

    def total(n, i):
        start, blocks = packets[n]
        mine = grads[blocks[i](group)].astype(jnp.float32)
        return (mine + x_in[start + i].astype(jnp.float32)).astype(jnp.bfloat16)

    def unless(condition, step):
        @pl.when(jnp.logical_not(condition))
        def _():
            step()

    def other(k):
        return lax.rem(me + k, shards)

    def in_copy(s, owner, source):
        return remote(
            summed.at[s, owner],
            gradient.at[place_of[s], source],
            in_send.at[s, owner],
            in_recv.at[s, source],
            (group, owner),
        )

    def out_copy(s, shard, source):
        spot = lax.rem(source, stride) * part + source // stride
        return remote(
            update.at[place_of[s], shard],
            result[s].at[spot],
            out_send.at[s, shard],
            out_recv.at[s, source],
            (group, shard),
        )

    def back_copy(s, j):
        from_rest = lax.rem(rest - j + stride, stride)
        span = pl.ds(from_rest * part, part)
        landing = pl.ds(s * shards + from_rest * part, part)
        n = s * stride + j
        return remote(result[s].at[span], back_in.at[landing], back_send.at[n], back_recv.at[n], partner)

    def scatter(s, first, last):
        for j in range(first, last):
            n = first_packet[s] + j
            x_copy(n).wait_recv()
            for i in range(part):
                summed[s, visited(j * part + i)] = total(n, i)
            for i in range(part):
                owner = visited(j * part + i)
                if j == 0:
                    unless(owner == me, in_copy(s, owner, me).start)
                else:
                    in_copy(s, owner, me).start()
        if first == 0:
            gradient[place_of[s], me] = summed[s, me]

    def spread(s):
        result[s][rest * part + ring] = update[place_of[s], me]
        for i in range(shards):
            if i < part:
                unless(visited(i) == me, out_copy(s, visited(i), me).start)
            else:
                out_copy(s, visited(i), me).start()

    def give_back(s):
        for j in range(stride):
            for q in range(part):
                source = q * stride + lax.rem(rest - j + stride, stride)
                if j == 0:
                    unless(source == me, out_copy(s, me, source).wait_recv)
                else:
                    out_copy(s, me, source).wait_recv()
            back_copy(s, j).start()
        for i in range(shards):
            settled[s * shards + i] = result[s][i]

    def ring_in_copy(q, source):
        return remote(
            heavy_sum.at[q],
            ring_in.at[source],
            ring_send.at[0, q],
            ring_recv.at[0, source],
            (group, q * stride + rest),
        )

    def near_in_copy(t, r, source):
        return remote(
            near_out.at[t, r],
            near_in.at[t, source],
            near_send.at[0, t, r],
            near_recv.at[0, t, source],
            (group, ring * stride + r),
        )

    def near_out_copy(t, r, source):
        return remote(
            far_out.at[t, r],
            far_in.at[t * stride + source],
            near_send.at[1, t, r],
            near_recv.at[1, t, source],
            (group, ring * stride + r),
        )

    def ring_out_copy(q, source):
        return remote(
            ring_out.at[q],
            heavy_result.at[source],
            ring_send.at[1, q],
            ring_recv.at[1, source],
            (group, q * stride + rest),
        )

    def heavy_back_copy(q):
        landing = pl.ds(light * shards + q * longest, size)
        n = light * stride + q
        return remote(heavy_result.at[q], back_in.at[landing], back_send.at[n], back_recv.at[n], partner)

    def ring_scatter(j):
        n = first_packet[light] + j
        x_copy(n).wait_recv()
        for i in range(size):
            heavy_sum[ring_at(j), i] = total(n, i)
        if offsets[j]:
            ring_in_copy(ring_at(j), ring).start()

    def near_scatter():
        ring_in[ring] = heavy_sum[ring]
        for j in range(part - 1):
            ring_in_copy(ring, ring_from(j)).wait_recv()
        for t in range(heavy):
            slot = group * levels + light + t
            for r in range(stride):
                place = table[1, slot * shards + ring * stride + r]
                for q in range(part):
                    near_out[t, r, q] = ring_in[q, place]
            for r in range(stride):
                unless(r == rest, near_in_copy(t, r, rest).start)
            near_in[t, rest] = near_out[t, rest]

    def near_spread(t):
        for r in range(stride):
            for q in range(part):
                far_out[t, r, q] = update[place_of[light + t], q * stride + r]
        for r in range(stride):
            unless(r == rest, near_out_copy(t, r, rest).start)
        far_in[t * stride + rest] = far_out[t, rest]

    def ring_spread():
        for t in range(heavy):
            for r in range(stride):
                unless(r == rest, near_out_copy(t, rest, r).wait_recv)
        for i in range(size):
            spot = table[3, (group * part + ring) * longest + i]
            for q in range(part):
                ring_out[q, i] = far_in[spot, q]
        for j in range(part - 1):
            ring_out_copy(ring_at(j), ring).start()
        heavy_result[ring] = ring_out[ring]
        heavy_back_copy(ring).start()

    def heavy_give_back():
        for j in range(part - 1):
            ring_out_copy(ring, ring_from(j)).wait_recv()
            heavy_back_copy(ring_from(j)).start()
        for q in range(part):
            for i in range(size):
                settled[light * shards + q * longest + i] = heavy_result[q, i]

    def ready(level):
        p = place_of[level]
        if level < light:

            @pl.loop(1, shards)
            def _(k):
                in_copy(level, me, other(k)).wait_recv()

        else:
            t = level - light
            for r in range(stride):
                unless(r == rest, near_in_copy(t, rest, r).wait_recv)
            for r in range(stride):
                for q in range(part):
                    gradient[p, q * stride + r] = near_in[t, r, q]
        for copy in stat_copies(level):
            copy.wait()

    half = stride // 2

    def before(p):
        if p == 0:
            for j in range(part):
                ring_scatter(j)
            near_scatter()
            scatter(0, 0, half + half // 2)

    def after(p):
        if p < heavy:
            near_spread(p)
            if p == 0:
                scatter(0, half + half // 2, stride)
                for s in range(1, light):
                    scatter(s, 0, half)
            if p == heavy - 1:
                for s in range(1, light):
                    scatter(s, half, stride)
        else:
            spread(p - heavy)
            if p == heavy:
                ring_spread()

    @pl.loop(0, levels)
    def _(step):
        for p, level in enumerate(sequence):

            @pl.when(step == p)
            def _():
                before(p)
                ready(level)

        block = gradient[step].reshape(shards * rows, width)
        update[step] = shape_block(block, left[step], right[step]).reshape(shards, rows, width)
        for p, level in enumerate(sequence):

            @pl.when(step == p)
            def _():
                after(p)

    give_back(0)
    heavy_give_back()
    for s in range(1, light):
        give_back(s)
    for s in range(light):
        for j in range(stride):
            back_copy(s, j).wait_recv()
        for i in range(shards):
            settled[side + s * shards + i] = back_in[s * shards + i]
        if s == 0:
            for q in range(part):
                heavy_back_copy(q).wait_recv()
                for i in range(size):
                    spot = light * shards + q * longest + i
                    settled[side + spot] = back_in[spot]
    for s in range(light):

        @pl.loop(1, shards)
        def _(k):
            in_copy(s, other(k), me).wait_send()
            out_copy(s, other(k), me).wait_send()

        for j in range(stride):
            back_copy(s, j).wait_send()
    for q in range(part):
        heavy_back_copy(q).wait_send()
        unless(q == ring, ring_in_copy(q, ring).wait_send)
        unless(q == ring, ring_out_copy(q, ring).wait_send)
    for t in range(heavy):
        for r in range(stride):
            unless(r == rest, near_in_copy(t, r, rest).wait_send)
            unless(r == rest, near_out_copy(t, r, rest).wait_send)
    for n in range(len(packets)):
        x_copy(n).wait_send()


def settle_kernel(table, settled, out):
    member = lax.axis_index("dp")
    for b in range(out.shape[0]):
        out[b] = settled[table[4 + member, b]]


def pair_body(group_grads, owners, stats_left, stats_right):
    shards = lax.axis_size("fsdp")
    _, blocks, rows, width = group_grads.shape
    levels = stats_left.shape[1]
    if levels == 1:
        return body(group_grads, owners, stats_left, stats_right)
    caps = level_caps(blocks, shards, 2 * levels, levels)
    light = min(sum(cap == shards for cap in caps), levels - 1)
    heavy = levels - light
    stride = stride_of(shards)
    part = shards // stride
    longest = stride * heavy
    fair = -(-sum(caps[light:]) // part)
    sizes = [size for size in range(max(1, fair - 2), fair + 1) if size < longest] + [longest]
    side = light * shards + part * longest
    dma = pltpu.SemaphoreType.DMA
    bf16 = jnp.bfloat16
    vmem = pl.BlockSpec(memory_space=pltpu.VMEM)
    smem = pl.BlockSpec(memory_space=pltpu.SMEM)
    hbm = pl.BlockSpec(memory_space=pltpu.HBM)

    def pieces(*shape):
        return pltpu.VMEM((*shape, rows, width), bf16)

    table = pl.pallas_call(
        functools.partial(table_kernel, light, heavy, shards),
        out_shape=jax.ShapeDtypeStruct((8, max(2 * levels * shards, blocks)), jnp.int32),
        in_specs=[vmem],
        out_specs=vmem,
    )(owners.reshape(1, blocks))
    packets = light * stride + part

    def fused(size, number):
        return pl.pallas_call(
            functools.partial(fused_kernel, light, size),
            out_shape=jax.ShapeDtypeStruct((2 * side, rows, width), bf16),
            in_specs=[hbm] * 4,
            out_specs=vmem,
            scratch_shapes=[
                pltpu.SMEM(table.shape, jnp.int32),
                pieces(blocks),
                pltpu.VMEM((levels, width, width), jnp.float32),
                pltpu.VMEM((levels, width, width), jnp.float32),
                pieces(light * shards + part * size),
                pieces(light * shards + part * size),
                pieces(light, shards),
                pieces(part, size),
                pieces(part, size),
                pieces(heavy, stride, part),
                pieces(heavy, stride, part),
                pieces(levels, shards),
                pieces(levels, shards),
                pieces(heavy, stride, part),
                pieces(heavy * stride, part),
                pieces(part, size),
                pieces(part, size),
                pieces(side),
                dma((2,)),
                dma((2, levels)),
                dma((packets,)),
                dma((packets,)),
                dma((light, shards)),
                dma((light, shards)),
                dma((light, shards)),
                dma((light, shards)),
                dma((2, part)),
                dma((2, part)),
                dma((2, heavy, stride)),
                dma((2, heavy, stride)),
                dma((packets,)),
                dma((packets,)),
            ]
            + [pieces(shards)] * light,
            compiler_params=pltpu.CompilerParams(
                collective_id=number, has_side_effects=True, vmem_limit_bytes=48 * 1024 * 1024
            ),
        )

    settle = pl.pallas_call(
        settle_kernel,
        out_shape=jax.ShapeDtypeStruct((blocks, rows, width), bf16),
        in_specs=[smem, vmem],
        out_specs=vmem,
        compiler_params=pltpu.CompilerParams(vmem_limit_bytes=16 * 1024 * 1024),
    )

    def with_lists(size, number):
        def run(table, *arrays):
            return settle(table, fused(size, number)(table, *arrays))

        return run

    length = table[6, 0]
    branch = sum((length > size).astype(jnp.int32) for size in sizes[:-1])
    return lax.switch(
        branch,
        [with_lists(size, number) for number, size in enumerate(sizes)],
        table,
        group_grads[0],
        stats_left[0],
        stats_right[0],
    )


def body(group_grads, owners, stats_left, stats_right):
    groups = lax.axis_size("dp")
    member = lax.axis_index("dp")
    shards = lax.axis_size("fsdp")
    per_member = stats_left.shape[1]
    capacity = per_member * groups
    owner_of, slot_of, positions = slot_table(owners)
    local = group_grads[0]
    total = local.astype(jnp.float32)
    for step in range(1, groups):
        total = total + shifted(local, groups, step).astype(jnp.float32)
    summed = total.astype(jnp.bfloat16)
    rows_here = summed.shape[1]
    block_width = summed.shape[2]
    wanted = member * per_member + jnp.arange(per_member, dtype=jnp.int32)
    targets = (jnp.arange(shards, dtype=jnp.int32)[:, None] * capacity + wanted[None, :]).reshape(
        -1
    )
    block_key = owner_of * capacity + slot_of
    matches = targets[:, None] == block_key[None, :]
    present = jnp.any(matches, axis=1)
    chosen = jnp.sum(jnp.where(matches, positions[None, :], 0), axis=1)
    outgoing = jnp.where(
        present[:, None, None], jnp.take(summed, chosen, axis=0), jnp.zeros((), jnp.bfloat16)
    )
    outgoing = outgoing.reshape(shards, per_member, rows_here, block_width)
    arrived = lax.all_to_all(outgoing, "fsdp", split_axis=0, concat_axis=2, tiled=True)
    gradient = arrived.reshape(per_member, block_width, block_width)
    update = shape_blocks(gradient, stats_left[0], stats_right[0])
    pieces = update.reshape(per_member, shards, rows_here, block_width)
    returned = lax.all_to_all(pieces, "fsdp", split_axis=1, concat_axis=0, tiled=True)
    returned = returned.reshape(shards * per_member, rows_here, block_width)
    mine = jnp.take(returned, owner_of * per_member + slot_of % per_member, axis=0)
    holder = slot_of // per_member
    result = mine
    for step in range(1, groups):
        theirs = (holder == (member - step) % groups)[:, None, None]
        result = jnp.where(theirs, shifted(mine, groups, step), result)
    return result


def solution(mesh):
    placed = (
        P("dp", None, "fsdp", None),
        P(),
        P("fsdp", "dp", None, None),
        P("fsdp", "dp", None, None),
    )
    return jax.shard_map(
        pair_body if mesh.shape["dp"] == 2 else body, mesh=mesh, in_specs=placed, out_specs=P(None, "fsdp", None), check_vma=False
    )
```

```python
import functools
import math
import jax
import jax.numpy as jnp
from jax import lax
from jax.experimental import pallas as pl
from jax.experimental.pallas import tpu as pltpu
from jax.sharding import PartitionSpec as P

ITERS = 2


BETA = 0.95

POWER = [math.comb(5, j) * 5.0 ** (5 - j) * (-1.0) ** j / 4.0**6 for j in range(6)]
COEF = [25.0 / 16.0, -5.0 / 16.0 - POWER[0]] + [-POWER[j] for j in range(1, 6)]


def mm(former, latter, dims=((1,), (0,))):
    return lax.dot_general(former, latter, (dims, ((), ())), preferred_element_type=jnp.float32)


def total_of(value):
    return jnp.sum(jnp.sum(value, axis=0, keepdims=True), axis=1, keepdims=True)


def newton_root(statistic):
    magnitude = jnp.sqrt(total_of(statistic * statistic) + 1e-06)
    first = statistic * (1.0 / magnitude)
    low_first = first.astype(jnp.bfloat16)
    second = mm(low_first, low_first)
    third = mm(second.astype(jnp.bfloat16), low_first)
    upper = COEF[4] * first + COEF[5] * second + COEF[6] * third
    lower = COEF[1] * first + COEF[2] * second + COEF[3] * third
    factor = lower + mm(third.astype(jnp.bfloat16), upper.astype(jnp.bfloat16))
    row = lax.broadcasted_iota(jnp.int32, factor.shape, 0)
    column = lax.broadcasted_iota(jnp.int32, factor.shape, 1)
    return (factor + jnp.where(row == column, COEF[0], 0.0)).astype(jnp.bfloat16)


def shape_kernel(gradient_ref, left_ref, right_ref, update_ref):
    gradient = gradient_ref[0]
    left_root = newton_root(BETA * left_ref[0] + mm(gradient, gradient, ((1,), (1,))))
    halfway = mm(left_root, gradient).astype(jnp.bfloat16)
    right_root = newton_root(BETA * right_ref[0] + mm(gradient, gradient, ((0,), (0,))))
    shaped = mm(halfway, right_root)
    wide = gradient.astype(jnp.float32)
    ratio = jnp.sqrt(total_of(wide * wide)) / jnp.sqrt(total_of(shaped * shaped) + 1e-06)
    update_ref[0] = (shaped * ratio).astype(jnp.bfloat16)


def shape_blocks(gradient, left, right, interpret=False):
    count, width, _ = gradient.shape
    spec = pl.BlockSpec((1, width, width), lambda k: (k, 0, 0))
    return pl.pallas_call(
        shape_kernel,
        grid=(count,),
        out_shape=jax.ShapeDtypeStruct(gradient.shape, jnp.bfloat16),
        in_specs=[spec] * 3,
        out_specs=spec,
        compiler_params=pltpu.CompilerParams(vmem_limit_bytes=48 * 1024 * 1024),
        cost_estimate=pl.CostEstimate(
            flops=20 * count * width**3, bytes_accessed=12 * count * width**2, transcendentals=0
        ),
        interpret=interpret,
    )(gradient, left, right)


def shifted(value, groups, step):
    return lax.ppermute(value, "dp", [(g, (g + step) % groups) for g in range(groups)])


def slot_table(owners):
    owner_of = owners[:, 0]
    positions = jnp.arange(owner_of.shape[0], dtype=jnp.int32)
    earlier = (owner_of[None, :] == owner_of[:, None]) & (positions[None, :] < positions[:, None])
    slot_of = jnp.sum(earlier.astype(jnp.int32), axis=1)
    return (owner_of, slot_of, positions)

MESH = pl.DeviceIdType.MESH


def shape_block(gradient, left, right):
    left_root = newton_root(BETA * left + mm(gradient, gradient, ((1,), (1,))))
    halfway = mm(left_root, gradient).astype(jnp.bfloat16)
    right_root = newton_root(BETA * right + mm(gradient, gradient, ((0,), (0,))))
    shaped = mm(halfway, right_root)
    wide = gradient.astype(jnp.float32)
    ratio = jnp.sqrt(total_of(wide * wide)) / jnp.sqrt(total_of(shaped * shaped) + 1e-06)
    return (shaped * ratio).astype(jnp.bfloat16)


def level_caps(blocks, shards, capacity, levels):
    caps = [shards]
    for slot in range(1, levels):
        caps.append(min(shards, (blocks - capacity + slot + 1 - shards) // slot))
    return caps


def stride_of(shards):
    return next(s for s in range(math.isqrt(shards), 0, -1) if shards % s == 0)


def table_kernel(light, heavy, shards, owners_ref, table_ref):
    blocks = owners_ref.shape[1]
    levels = light + heavy
    stride = stride_of(shards)
    part = shards // stride
    longest = stride * heavy

    def numbers(shape, axis):
        return lax.broadcasted_iota(jnp.int32, shape, axis).astype(jnp.float32)

    def split(value, size):
        quotient = jnp.floor((value + 0.5) * (1.0 / size))
        return quotient, value - size * quotient

    def down(mask, value=1.0):
        return jnp.sum(jnp.where(mask, value, 0.0), axis=0, keepdims=True)

    def across(mask, value=1.0):
        return jnp.sum(jnp.where(mask, value, 0.0), axis=1, keepdims=True)

    def listed(owner, slot):
        holder, depth = split(slot, levels)
        ring, rest = split(owner, stride)
        name = jnp.where(depth >= light, holder * part + ring, -1.0)
        return name, depth * stride + rest

    square = (blocks, blocks)
    first, second = numbers(square, 0), numbers(square, 1)
    owner_row = owners_ref[...].astype(jnp.float32)
    owner_col = across(first == second, owner_row)
    same = owner_col == owner_row
    slot_row = down(same & (first < second))
    slot_col = across(same & (second < first))
    list_row, key_row = listed(owner_row, slot_row)
    list_col, key_col = listed(owner_col, slot_col)
    together = list_col == list_row
    rank_row = down(together & (key_col < key_row))
    rank_col = across(together & (key_row < key_col))
    wide = (blocks, 2 * levels * shards)
    slot, owner = split(numbers(wide, 1), shards)
    at_owner = (slot_col == slot) & (owner_col == owner)
    block_col = numbers(wide, 0)
    lists = (blocks, 2 * part * longest)
    name, place = split(numbers(lists, 1), longest)
    at_place = (list_col == name) & (rank_col == place)
    rows = [
        down(at_owner, block_col),
        down(at_owner & (list_col >= 0.0), rank_col),
        down(at_place, numbers(lists, 0)),
        down(at_place, key_col - light * stride),
    ]
    for r, row in enumerate(rows):
        table_ref[r : r + 1, 0 : row.shape[1]] = row.astype(jnp.int32)
    holder, depth = split(slot_row, levels)
    ring, rest = split(owner_row, stride)
    near = jnp.where(
        list_row < 0.0,
        depth * shards + rest * part + ring,
        light * shards + ring * longest + rank_row,
    )
    side = light * shards + part * longest
    for member in range(2):
        pick = near + jnp.where(holder == member, 0.0, float(side))
        table_ref[4 + member : 5 + member, 0:blocks] = pick.astype(jnp.int32)
    length = jnp.max(jnp.where(list_row < 0.0, 0.0, rank_row + 1.0), axis=1, keepdims=True)
    table_ref[6:7, 0:1] = length.astype(jnp.int32)


def fused_kernel(
    light,
    size,
    table_hbm,
    grads_hbm,
    left_hbm,
    right_hbm,
    settled,
    table,
    grads,
    left,
    right,
    x_out,
    x_in,
    summed,
    heavy_sum,
    ring_in,
    near_out,
    near_in,
    gradient,
    update,
    far_out,
    far_in,
    ring_out,
    heavy_result,
    back_in,
    load_sem,
    stat_sem,
    x_send,
    x_recv,
    in_send,
    in_recv,
    out_send,
    out_recv,
    ring_send,
    ring_recv,
    near_send,
    near_recv,
    back_send,
    back_recv,
    *result,
):
    levels, shards, rows, width = gradient.shape
    heavy = levels - light
    stride = stride_of(shards)
    part = shards // stride
    longest = stride * heavy
    side = light * shards + part * longest
    group, me = lax.axis_index("dp"), lax.axis_index("fsdp")
    ring, rest = me // stride, lax.rem(me, stride)
    partner = (1 - group, me)
    sequence = [*range(light, levels), *range(light)]
    place_of = {level: p for p, level in enumerate(sequence)}

    def block_at(holder, s, owner):
        return table[0, (holder * levels + s) * shards + owner]

    def block_in(holder, q, i):
        return table[2, (holder * part + q) * longest + i]

    offsets = [*range(part // 2, part), *range(1, part // 2), 0]

    def ring_at(j):
        return lax.rem(ring + offsets[j], part)

    def ring_from(j):
        return lax.rem(ring - offsets[j] + part, part)

    def visited(i):
        return ring_at(i % part) * stride + lax.rem(rest + i // part, stride)

    def remote(source, target, send, recv, device):
        return pltpu.make_async_remote_copy(
            src_ref=source,
            dst_ref=target,
            send_sem=send,
            recv_sem=recv,
            device_id=device,
            device_id_type=MESH,
        )

    loads = [
        pltpu.make_async_copy(table_hbm, table, load_sem.at[0]),
        pltpu.make_async_copy(grads_hbm, grads, load_sem.at[1]),
    ]
    for copy in loads:
        copy.start()
    barrier = pltpu.get_barrier_semaphore()
    pl.semaphore_signal(barrier, inc=1, device_id=partner, device_id_type=MESH)

    @pl.loop(1, shards)
    def _(k):
        pl.semaphore_signal(
            barrier, inc=1, device_id=(group, lax.rem(me + k, shards)), device_id_type=MESH
        )

    def stat_copies(level):
        p = place_of[level]
        return [
            pltpu.make_async_copy(left_hbm.at[level], left.at[p], stat_sem.at[0, p]),
            pltpu.make_async_copy(right_hbm.at[level], right.at[p], stat_sem.at[1, p]),
        ]

    for level in sequence:
        for copy in stat_copies(level):
            copy.start()

    packets = []
    for level in sequence:
        if level < light:
            for j in range(stride):
                places = range(j * part, (j + 1) * part)
                packets.append(
                    (
                        level * shards + j * part,
                        [functools.partial(block_at, s=level, owner=visited(i)) for i in places],
                    )
                )
        elif level == light:
            for q in range(part):
                packets.append(
                    (
                        light * shards + q * size,
                        [functools.partial(block_in, q=ring_at(q), i=i) for i in range(size)],
                    )
                )
    first_packet = {}
    count = 0
    for level in sequence:
        if level <= light:
            first_packet[level] = count
            count += stride if level < light else part

    def x_copy(n):
        start, blocks = packets[n]
        span = pl.ds(start, len(blocks))
        return remote(x_out.at[span], x_in.at[span], x_send.at[n], x_recv.at[n], partner)

    def fill(n):
        start, blocks = packets[n]
        for i, block in enumerate(blocks):
            x_out[start + i] = grads[block(1 - group)]

    for copy in loads:
        copy.wait()
    fill(0)
    pl.semaphore_wait(barrier, shards)
    for n in range(len(packets)):
        x_copy(n).start()
        if n + 1 < len(packets):
            fill(n + 1)

    def total(n, i):
        start, blocks = packets[n]
        mine = grads[blocks[i](group)].astype(jnp.float32)
        return (mine + x_in[start + i].astype(jnp.float32)).astype(jnp.bfloat16)

    def unless(condition, step):
        @pl.when(jnp.logical_not(condition))
        def _():
            step()

    def other(k):
        return lax.rem(me + k, shards)

    def in_copy(s, owner, source):
        return remote(
            summed.at[s, owner],
            gradient.at[place_of[s], source],
            in_send.at[s, owner],
            in_recv.at[s, source],
            (group, owner),
        )

    def out_copy(s, shard, source):
        spot = lax.rem(source, stride) * part + source // stride
        return remote(
            update.at[place_of[s], shard],
            result[s].at[spot],
            out_send.at[s, shard],
            out_recv.at[s, source],
            (group, shard),
        )

    def back_copy(s, j):
        from_rest = lax.rem(rest - j + stride, stride)
        span = pl.ds(from_rest * part, part)
        landing = pl.ds(s * shards + from_rest * part, part)
        n = s * stride + j
        return remote(result[s].at[span], back_in.at[landing], back_send.at[n], back_recv.at[n], partner)

    def scatter(s, first, last):
        for j in range(first, last):
            n = first_packet[s] + j
            x_copy(n).wait_recv()
            for i in range(part):
                summed[s, visited(j * part + i)] = total(n, i)
            for i in range(part):
                owner = visited(j * part + i)
                if j == 0:
                    unless(owner == me, in_copy(s, owner, me).start)
                else:
                    in_copy(s, owner, me).start()
        if first == 0:
            gradient[place_of[s], me] = summed[s, me]

    def spread(s):
        result[s][rest * part + ring] = update[place_of[s], me]
        for i in range(shards):
            if i < part:
                unless(visited(i) == me, out_copy(s, visited(i), me).start)
            else:
                out_copy(s, visited(i), me).start()

    def give_back(s):
        for j in range(stride):
            for q in range(part):
                source = q * stride + lax.rem(rest - j + stride, stride)
                if j == 0:
                    unless(source == me, out_copy(s, me, source).wait_recv)
                else:
                    out_copy(s, me, source).wait_recv()
            back_copy(s, j).start()
        for i in range(shards):
            settled[s * shards + i] = result[s][i]

    def ring_in_copy(q, source):
        return remote(
            heavy_sum.at[q],
            ring_in.at[source],
            ring_send.at[0, q],
            ring_recv.at[0, source],
            (group, q * stride + rest),
        )

    def near_in_copy(t, r, source):
        return remote(
            near_out.at[t, r],
            near_in.at[t, source],
            near_send.at[0, t, r],
            near_recv.at[0, t, source],
            (group, ring * stride + r),
        )

    def near_out_copy(t, r, source):
        return remote(
            far_out.at[t, r],
            far_in.at[t * stride + source],
            near_send.at[1, t, r],
            near_recv.at[1, t, source],
            (group, ring * stride + r),
        )

    def ring_out_copy(q, source):
        return remote(
            ring_out.at[q],
            heavy_result.at[source],
            ring_send.at[1, q],
            ring_recv.at[1, source],
            (group, q * stride + rest),
        )

    def heavy_back_copy(q):
        landing = pl.ds(light * shards + q * longest, size)
        n = light * stride + q
        return remote(heavy_result.at[q], back_in.at[landing], back_send.at[n], back_recv.at[n], partner)

    def ring_scatter(j):
        n = first_packet[light] + j
        x_copy(n).wait_recv()
        for i in range(size):
            heavy_sum[ring_at(j), i] = total(n, i)
        if offsets[j]:
            ring_in_copy(ring_at(j), ring).start()

    def near_scatter():
        ring_in[ring] = heavy_sum[ring]
        for j in range(part - 1):
            ring_in_copy(ring, ring_from(j)).wait_recv()
        for t in range(heavy):
            slot = group * levels + light + t
            for r in range(stride):
                place = table[1, slot * shards + ring * stride + r]
                for q in range(part):
                    near_out[t, r, q] = ring_in[q, place]
            for r in range(stride):
                unless(r == rest, near_in_copy(t, r, rest).start)
            near_in[t, rest] = near_out[t, rest]

    def near_spread(t):
        for r in range(stride):
            for q in range(part):
                far_out[t, r, q] = update[place_of[light + t], q * stride + r]
        for r in range(stride):
            unless(r == rest, near_out_copy(t, r, rest).start)
        far_in[t * stride + rest] = far_out[t, rest]

    def ring_spread():
        for t in range(heavy):
            for r in range(stride):
                unless(r == rest, near_out_copy(t, rest, r).wait_recv)
        for i in range(size):
            spot = table[3, (group * part + ring) * longest + i]
            for q in range(part):
                ring_out[q, i] = far_in[spot, q]
        for j in range(part - 1):
            ring_out_copy(ring_at(j), ring).start()
        heavy_result[ring] = ring_out[ring]
        heavy_back_copy(ring).start()

    def heavy_give_back():
        for j in range(part - 1):
            ring_out_copy(ring, ring_from(j)).wait_recv()
            heavy_back_copy(ring_from(j)).start()
        for q in range(part):
            for i in range(size):
                settled[light * shards + q * longest + i] = heavy_result[q, i]

    def ready(level):
        p = place_of[level]
        if level < light:

            @pl.loop(1, shards)
            def _(k):
                in_copy(level, me, other(k)).wait_recv()

        else:
            t = level - light
            for r in range(stride):
                unless(r == rest, near_in_copy(t, rest, r).wait_recv)
            for r in range(stride):
                for q in range(part):
                    gradient[p, q * stride + r] = near_in[t, r, q]
        for copy in stat_copies(level):
            copy.wait()

    half = stride // 2

    def before(p):
        if p == 0:
            for j in range(part):
                ring_scatter(j)
            near_scatter()
            scatter(0, 0, half + half // 2)

    def after(p):
        if p < heavy:
            near_spread(p)
            if p == 0:
                scatter(0, half + half // 2, stride)
                for s in range(1, light):
                    scatter(s, 0, half + half // 2)
            if p == heavy - 1:
                for s in range(1, light):
                    scatter(s, half + half // 2, stride)
        else:
            spread(p - heavy)
            if p == heavy:
                ring_spread()

    @pl.loop(0, levels)
    def _(step):
        for p, level in enumerate(sequence):

            @pl.when(step == p)
            def _():
                before(p)
                ready(level)

        block = gradient[step].reshape(shards * rows, width)
        update[step] = shape_block(block, left[step], right[step]).reshape(shards, rows, width)
        for p, level in enumerate(sequence):

            @pl.when(step == p)
            def _():
                after(p)

    give_back(0)
    heavy_give_back()
    for s in range(1, light):
        give_back(s)
    for s in range(light):
        for j in range(stride):
            back_copy(s, j).wait_recv()
        for i in range(shards):
            settled[side + s * shards + i] = back_in[s * shards + i]
        if s == 0:
            for q in range(part):
                heavy_back_copy(q).wait_recv()
                for i in range(size):
                    spot = light * shards + q * longest + i
                    settled[side + spot] = back_in[spot]
    for s in range(light):

        @pl.loop(1, shards)
        def _(k):
            in_copy(s, other(k), me).wait_send()
            out_copy(s, other(k), me).wait_send()

        for j in range(stride):
            back_copy(s, j).wait_send()
    for q in range(part):
        heavy_back_copy(q).wait_send()
        unless(q == ring, ring_in_copy(q, ring).wait_send)
        unless(q == ring, ring_out_copy(q, ring).wait_send)
    for t in range(heavy):
        for r in range(stride):
            unless(r == rest, near_in_copy(t, r, rest).wait_send)
            unless(r == rest, near_out_copy(t, r, rest).wait_send)
    for n in range(len(packets)):
        x_copy(n).wait_send()


def settle_kernel(table, settled, out):
    member = lax.axis_index("dp")
    for b in range(out.shape[0]):
        out[b] = settled[table[4 + member, b]]


def pair_body(group_grads, owners, stats_left, stats_right):
    shards = lax.axis_size("fsdp")
    _, blocks, rows, width = group_grads.shape
    levels = stats_left.shape[1]
    if levels == 1:
        return body(group_grads, owners, stats_left, stats_right)
    caps = level_caps(blocks, shards, 2 * levels, levels)
    light = min(sum(cap == shards for cap in caps), levels - 1)
    heavy = levels - light
    stride = stride_of(shards)
    part = shards // stride
    longest = stride * heavy
    fair = -(-sum(caps[light:]) // part)
    sizes = [size for size in range(max(1, fair - 2), fair + 1) if size < longest] + [longest]
    side = light * shards + part * longest
    dma = pltpu.SemaphoreType.DMA
    bf16 = jnp.bfloat16
    vmem = pl.BlockSpec(memory_space=pltpu.VMEM)
    smem = pl.BlockSpec(memory_space=pltpu.SMEM)
    hbm = pl.BlockSpec(memory_space=pltpu.HBM)

    def pieces(*shape):
        return pltpu.VMEM((*shape, rows, width), bf16)

    table = pl.pallas_call(
        functools.partial(table_kernel, light, heavy, shards),
        out_shape=jax.ShapeDtypeStruct((8, max(2 * levels * shards, blocks)), jnp.int32),
        in_specs=[vmem],
        out_specs=vmem,
    )(owners.reshape(1, blocks))
    packets = light * stride + part

    def fused(size, number):
        return pl.pallas_call(
            functools.partial(fused_kernel, light, size),
            out_shape=jax.ShapeDtypeStruct((2 * side, rows, width), bf16),
            in_specs=[hbm] * 4,
            out_specs=vmem,
            scratch_shapes=[
                pltpu.SMEM(table.shape, jnp.int32),
                pieces(blocks),
                pltpu.VMEM((levels, width, width), jnp.float32),
                pltpu.VMEM((levels, width, width), jnp.float32),
                pieces(light * shards + part * size),
                pieces(light * shards + part * size),
                pieces(light, shards),
                pieces(part, size),
                pieces(part, size),
                pieces(heavy, stride, part),
                pieces(heavy, stride, part),
                pieces(levels, shards),
                pieces(levels, shards),
                pieces(heavy, stride, part),
                pieces(heavy * stride, part),
                pieces(part, size),
                pieces(part, size),
                pieces(side),
                dma((2,)),
                dma((2, levels)),
                dma((packets,)),
                dma((packets,)),
                dma((light, shards)),
                dma((light, shards)),
                dma((light, shards)),
                dma((light, shards)),
                dma((2, part)),
                dma((2, part)),
                dma((2, heavy, stride)),
                dma((2, heavy, stride)),
                dma((packets,)),
                dma((packets,)),
            ]
            + [pieces(shards)] * light,
            compiler_params=pltpu.CompilerParams(
                collective_id=number, has_side_effects=True, vmem_limit_bytes=48 * 1024 * 1024
            ),
        )

    settle = pl.pallas_call(
        settle_kernel,
        out_shape=jax.ShapeDtypeStruct((blocks, rows, width), bf16),
        in_specs=[smem, vmem],
        out_specs=vmem,
        compiler_params=pltpu.CompilerParams(vmem_limit_bytes=16 * 1024 * 1024),
    )

    def with_lists(size, number):
        def run(table, *arrays):
            return settle(table, fused(size, number)(table, *arrays))

        return run

    length = table[6, 0]
    branch = sum((length > size).astype(jnp.int32) for size in sizes[:-1])
    return lax.switch(
        branch,
        [with_lists(size, number) for number, size in enumerate(sizes)],
        table,
        group_grads[0],
        stats_left[0],
        stats_right[0],
    )


def body(group_grads, owners, stats_left, stats_right):
    groups = lax.axis_size("dp")
    member = lax.axis_index("dp")
    shards = lax.axis_size("fsdp")
    per_member = stats_left.shape[1]
    capacity = per_member * groups
    owner_of, slot_of, positions = slot_table(owners)
    local = group_grads[0]
    total = local.astype(jnp.float32)
    for step in range(1, groups):
        total = total + shifted(local, groups, step).astype(jnp.float32)
    summed = total.astype(jnp.bfloat16)
    rows_here = summed.shape[1]
    block_width = summed.shape[2]
    wanted = member * per_member + jnp.arange(per_member, dtype=jnp.int32)
    targets = (jnp.arange(shards, dtype=jnp.int32)[:, None] * capacity + wanted[None, :]).reshape(
        -1
    )
    block_key = owner_of * capacity + slot_of
    matches = targets[:, None] == block_key[None, :]
    present = jnp.any(matches, axis=1)
    chosen = jnp.sum(jnp.where(matches, positions[None, :], 0), axis=1)
    outgoing = jnp.where(
        present[:, None, None], jnp.take(summed, chosen, axis=0), jnp.zeros((), jnp.bfloat16)
    )
    outgoing = outgoing.reshape(shards, per_member, rows_here, block_width)
    arrived = lax.all_to_all(outgoing, "fsdp", split_axis=0, concat_axis=2, tiled=True)
    gradient = arrived.reshape(per_member, block_width, block_width)
    update = shape_blocks(gradient, stats_left[0], stats_right[0])
    pieces = update.reshape(per_member, shards, rows_here, block_width)
    returned = lax.all_to_all(pieces, "fsdp", split_axis=1, concat_axis=0, tiled=True)
    returned = returned.reshape(shards * per_member, rows_here, block_width)
    mine = jnp.take(returned, owner_of * per_member + slot_of % per_member, axis=0)
    holder = slot_of // per_member
    result = mine
    for step in range(1, groups):
        theirs = (holder == (member - step) % groups)[:, None, None]
        result = jnp.where(theirs, shifted(mine, groups, step), result)
    return result


def solution(mesh):
    placed = (
        P("dp", None, "fsdp", None),
        P(),
        P("fsdp", "dp", None, None),
        P("fsdp", "dp", None, None),
    )
    return jax.shard_map(
        pair_body if mesh.shape["dp"] == 2 else body, mesh=mesh, in_specs=placed, out_specs=P(None, "fsdp", None), check_vma=False
    )
```
